128 devices in a mesh: dp: 8 (over z, core), tensor: 16 (over y, x).
Axes of the slice: x: 4, y: 4, z: 4, core: 2. Of those that a mesh axis runs over, the one named last changes fastest.
Arguments:
- embed_rows: bfloat16 [196608, 1024], P('tensor', 'dp'), may hold values from -6 to 6
- head_rows: bfloat16 [196608, 1024], P('tensor', 'dp'), may hold values from -6 to 6
- row_offsets: int32 [2, 17], replicated, may hold values from -2047 to 133119, as said below
- slot_table: int32 [2048], replicated, may hold values from 0 to 2047, as said below
- probe: bfloat16 [1024, 1024], replicated, may hold values from -0.1875 to 0.1875
Outputs:
- stored: bfloat16 [2048, 128, 1024], P(('dp', 'tensor'))
- sketch: float32 [2048, 128, 1024], P(('dp', 'tensor'))
The draws below stay inside these ranges and needn't reach their ends.
Inputs may be any that keep to these rules, and one draw needn't show every extreme that they name: row_offsets[m, 16] is row_offsets[m, 0] + 131072; every entry row_offsets[m, t] with t < 16 lies strictly within 2048 rows of t * 8192, and the distance 8192 // 4 - 1 is reached above and below among ranks 1 onward in every row of every draw; row_offsets[m, 0] is never 0, above 0 for one matrix and below 0 for the other. `slot_table`: A permutation of the 2048 block numbers. Devices along dp+tensor write 16 consecutive slots each; among one device's slots exactly 1 block come from each aligned range of 8192 vocabulary rows (rows t * 8192 onward of either matrix, both matrices together).
All inputs are finite; a program needn't handle non-finite values.
Results may differ from the reference program's by a relative error of at most 0.001.
Values may be sent and summed in bfloat16 or wider, within the bound.
A program may use at most 64 MiB of HBM per device.

```python
import jax
import jax.numpy as jnp
from jax import lax

R = 8192
PW = 1024
BLOCK = 128
CAP = 12288
C = 1024
NBLK = 1024
N_TENSOR = 16
DEVICES = 128


def draw_row_offsets(key, part):
    first, second, third, fourth, fifth = jax.random.split(key, 5)
    reach = R // 4 - 1
    inner = N_TENSOR - 1
    shifts = jax.random.randint(first, (2, inner), -reach, reach + 1)
    upper = jax.random.randint(second, (2,), 0, inner)
    lower = (upper + 1 + jax.random.randint(third, (2,), 0, inner - 1)) % inner
    column = jnp.arange(inner)[None, :]
    shifts = jnp.where(column == upper[:, None], reach, shifts)
    shifts = jnp.where(column == lower[:, None], -reach, shifts)
    interior = jnp.arange(1, N_TENSOR)[None, :] * R + shifts
    size = jax.random.randint(fourth, (2,), 1, reach + 1)
    flip = jax.random.randint(fifth, (), 0, 2)
    signs = jnp.where(jnp.arange(2) == flip, 1, -1)
    starts = (signs * size).astype(jnp.int32)[:, None]
    ends = starts + R * N_TENSOR
    return jnp.concatenate([starts, interior.astype(jnp.int32), ends], axis=1).astype(jnp.int32)


def draw_slot_table(key, part):
    first, second = jax.random.split(key)
    per_rank = R // BLOCK
    total_blocks = per_rank * N_TENSOR
    slot_count = 2 * total_blocks // DEVICES
    shuffled = jax.random.permutation(first, DEVICES).astype(jnp.int32)
    source = (shuffled[:, None] + jnp.arange(slot_count, dtype=jnp.int32)[None, :]) % N_TENSOR
    flat_source = source.reshape(-1)
    slot_total = DEVICES * slot_count
    noise = jax.random.permutation(second, slot_total).astype(jnp.int32)
    ordering = jnp.argsort(flat_source * slot_total + noise)
    within = jnp.arange(slot_total, dtype=jnp.int32) % (2 * per_rank)
    local_block = jnp.zeros((slot_total,), jnp.int32).at[ordering].set(within)
    result = local_block // per_rank * total_blocks + flat_source * per_rank + local_block % per_rank
    return result.astype(jnp.int32)


def steps_of(own_key, extent, pieces, least, high):
    level = 1.0
    for position, parts in pieces:
        draws = jax.random.uniform(jax.random.fold_in(jax.random.fold_in(own_key, 6), position), (parts,), jnp.float32, least / len(pieces), high / len(pieces))
        level = level * jnp.repeat(jnp.exp(draws), extent[position] // parts).reshape((-1,) + (1,) * (len(extent) - 1 - position))
    return level


def normal_values(own_key, extent, scale, bound, cuts=(), kind=jnp.bfloat16):
    gain = steps_of(own_key, extent, cuts, -0.22, 0.18) if cuts else 1.0
    array = jax.random.normal(own_key, extent, jnp.float32) * scale * gain
    return jnp.minimum(jnp.maximum(array, -bound), bound).astype(kind)


def setup_inputs(seed: int = 0) -> dict:
    seeds = jax.random.split(jax.random.key(seed), 6)
    embed_rows = normal_values(seeds[0], (N_TENSOR * CAP, C), 1.0, 6.0, ((0, 16), (1, 8)))
    head_rows = normal_values(seeds[1], (N_TENSOR * CAP, C), 1.0, 6.0, ((0, 16), (1, 8)))
    row_offsets = draw_row_offsets(jax.random.fold_in(seeds[5], 71), 0)
    slot_table = draw_slot_table(jax.random.fold_in(seeds[5], 71), 0)
    probe = normal_values(seeds[4], (C, PW), C ** -0.5, 0.1875)
    return dict(embed_rows=embed_rows, head_rows=head_rows, row_offsets=row_offsets, slot_table=slot_table, probe=probe)


def assemble(buffer, offsets):
    vocab_rows = jnp.arange(R * N_TENSOR, dtype=jnp.int32)
    unwrapped = jnp.where(vocab_rows < offsets[0], vocab_rows + R * N_TENSOR,
                          jnp.where(vocab_rows >= offsets[N_TENSOR], vocab_rows - R * N_TENSOR, vocab_rows)).astype(jnp.int32)
    owner = jnp.sum((offsets[1:N_TENSOR][None, :] <= unwrapped[:, None]).astype(jnp.int32), axis=1).astype(jnp.int32)
    source_row = (owner * CAP + unwrapped - offsets[owner]).astype(jnp.int32)
    return buffer[source_row]


def reference(embed_rows, head_rows, row_offsets, slot_table, probe):
    whole = jnp.concatenate([assemble(embed_rows, row_offsets[0]), assemble(head_rows, row_offsets[1])], axis=0)
    blocks = whole.reshape(2 * NBLK, BLOCK, C)
    stored = blocks[slot_table]
    sketch = jnp.dot(stored.reshape(-1, C).astype(jnp.float32), probe.astype(jnp.float32),
                     precision=lax.Precision.HIGHEST, preferred_element_type=jnp.float32)
    return stored, sketch.reshape(2 * NBLK, BLOCK, PW)
```

```python
import functools

import jax
import jax.numpy as jnp
from jax import lax
from jax.experimental import pallas as pl
from jax.experimental.pallas import tpu as pltpu
from jax.sharding import PartitionSpec as P

R = 8192
BLOCK = 128
GROUP = 8


def from_behind(block, axis, distance):
    devices = range(lax.axis_size(axis))
    route = [((i - distance) % len(devices), i) for i in devices]
    return lax.ppermute(block, axis, route)


def own_kernel(quarter, before, dest, embed, head, out, ext, wide, packed, load_sem, store_sem):
    rows = GROUP * BLOCK
    groups = R // rows
    chunks = (R + quarter) // rows
    per_rank = R // BLOCK
    for m, source in enumerate((embed, head)):
        for c in range(chunks):
            pltpu.make_async_copy(
                source.at[pl.ds(c * rows, rows)],
                ext.at[m, pl.ds(quarter + c * rows, rows)],
                load_sem.at[m, c],
            ).start()
    ahead = quarter // rows
    for m, source in enumerate((embed, head)):
        for g in range(groups):
            for c in range(chunks):
                if c == g + ahead or (g == 0 and c < ahead):
                    pltpu.make_async_copy(
                        source.at[pl.ds(c * rows, rows)],
                        ext.at[m, pl.ds(quarter + c * rows, rows)],
                        load_sem.at[m, c],
                    ).wait()
            start = quarter + g * rows - before[m]
            aligned = start // 16 * 16
            offset = start - aligned
            slot = g % 2
            wide[slot] = ext[m, pl.ds(pl.multiple_of(aligned, 16), rows + 16), :].astype(jnp.float32)
            first = m * per_rank + g * GROUP
            packed[pl.ds(first * BLOCK, rows), :] = wide[slot, pl.ds(offset, rows), :].astype(jnp.bfloat16)
            for b in range(GROUP):
                block = first + b
                pltpu.make_async_copy(
                    packed.at[pl.ds(block * BLOCK, BLOCK)], out.at[dest[block]], store_sem.at[block]
                ).start()

    @pl.loop(0, 2 * per_rank)
    def _(block):
        pltpu.make_async_copy(
            packed.at[pl.ds(0, BLOCK)], out.at[dest[block]], store_sem.at[block]
        ).wait()


def pack_own(embed_rows, head_rows, before, dest, quarter):
    blocks = 2 * (R // BLOCK)
    rows = GROUP * BLOCK
    width = embed_rows.shape[1]
    chunks = (R + quarter) // rows
    return pl.pallas_call(
        functools.partial(own_kernel, quarter),
        grid_spec=pltpu.PrefetchScalarGridSpec(
            num_scalar_prefetch=2,
            grid=(),
            in_specs=[pl.BlockSpec(memory_space=pl.ANY)] * 2,
            out_specs=pl.BlockSpec(memory_space=pl.ANY),
            scratch_shapes=[
                pltpu.VMEM((2, R + 2 * quarter + rows, width), jnp.bfloat16),
                pltpu.VMEM((2, rows + 16, width), jnp.float32),
                pltpu.VMEM((blocks * BLOCK, width), jnp.bfloat16),
                pltpu.SemaphoreType.DMA((2, chunks)),
                pltpu.SemaphoreType.DMA((blocks,)),
            ],
        ),
        out_shape=jax.ShapeDtypeStruct((blocks, BLOCK, width), embed_rows.dtype),
        cost_estimate=pl.CostEstimate(flops=0, bytes_accessed=10 << 20, transcendentals=0),
    )(before, dest, embed_rows, head_rows)


def patch_kernel(quarter, before, after, dest, left, right, _, out, lbuf, rbuf, wide, edge, packed,
                 load_sem, edge_sem, store_sem):
    per_rank = R // BLOCK
    most = quarter // BLOCK + 1
    lead = BLOCK

    def load_left(m):
        return pltpu.make_async_copy(left.at[m], lbuf.at[m], load_sem.at[0, m])

    def load_right(m):
        return pltpu.make_async_copy(right.at[m], rbuf.at[m], load_sem.at[1, m])

    def load_edge(side, m, block):
        return pltpu.make_async_copy(out.at[dest[block]], edge.at[side, m], edge_sem.at[side, m])

    def store(side, m, i, block):
        return pltpu.make_async_copy(
            packed.at[side, m, i], out.at[dest[block]], store_sem.at[side, m, i]
        )

    row = lax.broadcasted_iota(jnp.int32, (BLOCK, lbuf.shape[-1]), 0)
    counts = []
    for m in range(2):
        n_left = (jnp.maximum(before[m], 0) + BLOCK - 1) // BLOCK
        first = jnp.minimum(after[m] // BLOCK, per_rank)
        n_right = per_rank - first
        counts.append((n_left, first, n_right))

        @pl.when(n_left > 0)
        def _():
            load_left(m).start()
            load_edge(0, m, m * per_rank + n_left - 1).start()

        @pl.when(n_right > 0)
        def _():
            load_right(m).start()
            load_edge(1, m, m * per_rank + first).start()

    for m in range(2):
        n_left, first, n_right = counts[m]

        @pl.when(n_left > 0)
        def _():
            load_left(m).wait()
            load_edge(0, m, m * per_rank + n_left - 1).wait()

            @pl.loop(0, n_left)
            def _(i):
                x = lbuf[m, pl.ds(pl.multiple_of(i * BLOCK, BLOCK), BLOCK), :].astype(jnp.float32)
                keep = edge[0, m].astype(jnp.float32)
                x = jnp.where(row + i * BLOCK < before[m], x, keep)
                packed[0, m, i] = x.astype(jnp.bfloat16)
                store(0, m, i, m * per_rank + i).start()

        @pl.when(n_right > 0)
        def _():
            load_right(m).wait()
            load_edge(1, m, m * per_rank + first).wait()
            wide[m, pl.ds(lead, quarter), :] = rbuf[m].astype(jnp.float32)
            skip = after[m] - first * BLOCK

            @pl.loop(0, n_right)
            def _(i):
                x = wide[m, pl.ds(lead + i * BLOCK - skip, BLOCK), :]
                keep = edge[1, m].astype(jnp.float32)
                x = jnp.where(row + i * BLOCK >= skip, x, keep)
                packed[1, m, i] = x.astype(jnp.bfloat16)
                store(1, m, i, m * per_rank + first + i).start()

    for m in range(2):
        n_left, first, n_right = counts[m]

        @pl.loop(0, n_left)
        def _(i):
            store(0, m, i, m * per_rank + i).wait()

        @pl.loop(0, n_right)
        def _(i):
            store(1, m, i, m * per_rank + first + i).wait()


def patch(outgoing, left, right, before, after, dest):
    quarter, width = left.shape[1:]
    most = quarter // BLOCK + 1
    dtype = outgoing.dtype
    return pl.pallas_call(
        functools.partial(patch_kernel, quarter),
        grid_spec=pltpu.PrefetchScalarGridSpec(
            num_scalar_prefetch=3,
            grid=(),
            in_specs=[pl.BlockSpec(memory_space=pl.ANY)] * 3,
            out_specs=pl.BlockSpec(memory_space=pl.ANY),
            scratch_shapes=[
                pltpu.VMEM((2, quarter, width), dtype),
                pltpu.VMEM((2, quarter, width), dtype),
                pltpu.VMEM((2, quarter + 2 * BLOCK, width), jnp.float32),
                pltpu.VMEM((2, 2, BLOCK, width), dtype),
                pltpu.VMEM((2, 2, most, BLOCK, width), dtype),
                pltpu.SemaphoreType.DMA((2, 2)),
                pltpu.SemaphoreType.DMA((2, 2)),
                pltpu.SemaphoreType.DMA((2, 2, most)),
            ],
        ),
        out_shape=jax.ShapeDtypeStruct(outgoing.shape, dtype),
        input_output_aliases={5: 0},
        cost_estimate=pl.CostEstimate(flops=0, bytes_accessed=6 << 20, transcendentals=0),
    )(before, after, dest, left, right, outgoing)


PAIR = 2


def finish_kernel(source, *refs):
    pieces = refs[:PAIR]
    probe, stored, sketch = refs[PAIR:]
    n_data, height, width = pieces[0].shape
    for i in range(PAIR):
        for d in range(n_data):
            stored[i, :, d * width:(d + 1) * width] = pieces[i][d]
    x = stored[...].reshape(PAIR * height, n_data * width)
    y = jnp.dot(x, probe[...], preferred_element_type=jnp.float32)
    sketch[...] = y.reshape(sketch.shape)


def finish(incoming, probe, source):
    n_data, n_tensor, height, width = incoming.shape
    slots = source.shape[0]
    columns = n_data * width

    def piece(i):
        return pl.BlockSpec(
            (n_data, None, height, width), lambda g, source: (0, source[g * PAIR + i], 0, 0)
        )

    return pl.pallas_call(
        finish_kernel,
        grid_spec=pltpu.PrefetchScalarGridSpec(
            num_scalar_prefetch=1,
            grid=(slots // PAIR,),
            in_specs=[piece(i) for i in range(PAIR)]
            + [pl.BlockSpec(probe.shape, lambda g, source: (0, 0))],
            out_specs=[
                pl.BlockSpec((PAIR, height, columns), lambda g, source: (g, 0, 0)),
                pl.BlockSpec((PAIR, height, probe.shape[1]), lambda g, source: (g, 0, 0)),
            ],
        ),
        out_shape=[
            jax.ShapeDtypeStruct((slots, height, columns), incoming.dtype),
            jax.ShapeDtypeStruct((slots, height, probe.shape[1]), jnp.float32),
        ],
        cost_estimate=pl.CostEstimate(
            flops=2 * slots * height * columns * probe.shape[1],
            bytes_accessed=18 << 20,
            transcendentals=0,
        ),
    )(source, *([incoming] * PAIR), probe)


def shards(embed_rows, head_rows, row_offsets, slot_table, probe):
    n_tensor = lax.axis_size("tensor")
    n_data = lax.axis_size("dp")
    my_tensor = lax.axis_index("tensor")
    my_data = lax.axis_index("dp")
    quarter = R // 4
    height, width = embed_rows.shape
    buffers = [embed_rows, head_rows]
    own_start = row_offsets[:, my_tensor]
    next_start = row_offsets[:, my_tensor + 1]
    before = own_start - my_tensor * R
    after = next_start - my_tensor * R
    lead_part = jnp.stack([embed_rows[:quarter], head_rows[:quarter]])
    tail_begin = jnp.clip((my_tensor + 1) * R - own_start, 0, height - quarter)
    trail_part = jnp.stack(
        [lax.dynamic_slice_in_dim(buffers[m], tail_begin[m], quarter, 0) for m in range(2)]
    )
    from_right = from_behind(lead_part, "tensor", -1)
    from_left = from_behind(trail_part, "tensor", 1)

    devices = n_tensor * n_data
    per_rank = R // BLOCK
    total_blocks = per_rank * n_tensor
    slot_count = 2 * total_blocks // devices
    local = jnp.arange(2 * per_rank, dtype=jnp.int32)
    number = local // per_rank * total_blocks + my_tensor * per_rank + local % per_rank
    holder = jnp.arange(2 * total_blocks, dtype=jnp.int32) // slot_count
    dest = jnp.sum(jnp.where(slot_table[None, :] == number[:, None], holder[None, :], 0), axis=1)
    dest = dest.astype(jnp.int32)

    outgoing = pack_own(embed_rows, head_rows, before, dest, quarter)
    outgoing = patch(outgoing, from_left, from_right, before, after, dest)
    incoming = lax.all_to_all(outgoing, ("dp", "tensor"), split_axis=0, concat_axis=0, tiled=True)
    writer = my_data * n_tensor + my_tensor
    mine = lax.dynamic_slice_in_dim(slot_table, writer * slot_count, slot_count)
    source = mine % total_blocks // per_rank
    incoming = incoming.reshape(n_data, n_tensor, BLOCK, width)
    stored, sketch = finish(incoming, probe, source)
    return (stored, sketch)


def solution(mesh):
    return jax.shard_map(
        shards,
        mesh=mesh,
        in_specs=(P("tensor", "dp"), P("tensor", "dp"), P(), P(), P()),
        out_specs=(P(("dp", "tensor"), None, None), P(("dp", "tensor"), None, None)),
        check_vma=False,
    )
```

```python
import functools
import itertools
import random

import jax
import jax.numpy as jnp
from jax import lax
from jax.experimental import pallas as pl
from jax.experimental.pallas import tpu as pltpu
from jax.sharding import PartitionSpec as P

R = 8192
BLOCK = 128
GROUP = 8


def from_behind(block, axis, distance):
    devices = range(lax.axis_size(axis))
    route = [((i - distance) % len(devices), i) for i in devices]
    return lax.ppermute(block, axis, route)


def own_kernel(quarter, before, dest, embed, head, out, ext, wide, packed, load_sem, store_sem):
    rows = GROUP * BLOCK
    groups = R // rows
    chunks = (R + quarter) // rows
    per_rank = R // BLOCK
    for m, source in enumerate((embed, head)):
        for c in range(chunks):
            pltpu.make_async_copy(
                source.at[pl.ds(c * rows, rows)],
                ext.at[m, pl.ds(quarter + c * rows, rows)],
                load_sem.at[m, c],
            ).start()
    ahead = quarter // rows
    for m, source in enumerate((embed, head)):
        for g in range(groups):
            for c in range(chunks):
                if c == g + ahead or (g == 0 and c < ahead):
                    pltpu.make_async_copy(
                        source.at[pl.ds(c * rows, rows)],
                        ext.at[m, pl.ds(quarter + c * rows, rows)],
                        load_sem.at[m, c],
                    ).wait()
            start = quarter + g * rows - before[m]
            aligned = start // 16 * 16
            offset = start - aligned
            slot = g % 2
            wide[slot] = ext[m, pl.ds(pl.multiple_of(aligned, 16), rows + 16), :].astype(jnp.float32)
            first = m * per_rank + g * GROUP
            packed[pl.ds(first * BLOCK, rows), :] = wide[slot, pl.ds(offset, rows), :].astype(jnp.bfloat16)
            for b in range(GROUP):
                block = first + b
                pltpu.make_async_copy(
                    packed.at[pl.ds(block * BLOCK, BLOCK)], out.at[dest[block]], store_sem.at[block]
                ).start()

    @pl.loop(0, 2 * per_rank)
    def _(block):
        pltpu.make_async_copy(
            packed.at[pl.ds(0, BLOCK)], out.at[dest[block]], store_sem.at[block]
        ).wait()


def pack_own(embed_rows, head_rows, before, dest, quarter):
    blocks = 2 * (R // BLOCK)
    rows = GROUP * BLOCK
    width = embed_rows.shape[1]
    chunks = (R + quarter) // rows
    return pl.pallas_call(
        functools.partial(own_kernel, quarter),
        grid_spec=pltpu.PrefetchScalarGridSpec(
            num_scalar_prefetch=2,
            grid=(),
            in_specs=[pl.BlockSpec(memory_space=pl.ANY)] * 2,
            out_specs=pl.BlockSpec(memory_space=pl.ANY),
            scratch_shapes=[
                pltpu.VMEM((2, R + 2 * quarter + rows, width), jnp.bfloat16),
                pltpu.VMEM((2, rows + 16, width), jnp.float32),
                pltpu.VMEM((blocks * BLOCK, width), jnp.bfloat16),
                pltpu.SemaphoreType.DMA((2, chunks)),
                pltpu.SemaphoreType.DMA((blocks,)),
            ],
        ),
        out_shape=jax.ShapeDtypeStruct((blocks, BLOCK, width), embed_rows.dtype),
        cost_estimate=pl.CostEstimate(flops=0, bytes_accessed=10 << 20, transcendentals=0),
    )(before, dest, embed_rows, head_rows)


def patch_kernel(quarter, before, after, dest, left, right, _, out, lbuf, rbuf, wide, edge, packed,
                 load_sem, edge_sem, store_sem):
    per_rank = R // BLOCK
    most = quarter // BLOCK + 1
    lead = BLOCK

    def load_left(m):
        return pltpu.make_async_copy(left.at[m], lbuf.at[m], load_sem.at[0, m])

    def load_right(m):
        return pltpu.make_async_copy(right.at[m], rbuf.at[m], load_sem.at[1, m])

    def load_edge(side, m, block):
        return pltpu.make_async_copy(out.at[dest[block]], edge.at[side, m], edge_sem.at[side, m])

    def store(side, m, i, block):
        return pltpu.make_async_copy(
            packed.at[side, m, i], out.at[dest[block]], store_sem.at[side, m, i]
        )

    row = lax.broadcasted_iota(jnp.int32, (BLOCK, lbuf.shape[-1]), 0)
    counts = []
    for m in range(2):
        n_left = (jnp.maximum(before[m], 0) + BLOCK - 1) // BLOCK
        first = jnp.minimum(after[m] // BLOCK, per_rank)
        n_right = per_rank - first
        counts.append((n_left, first, n_right))

        @pl.when(n_left > 0)
        def _():
            load_left(m).start()
            load_edge(0, m, m * per_rank + n_left - 1).start()

        @pl.when(n_right > 0)
        def _():
            load_right(m).start()
            load_edge(1, m, m * per_rank + first).start()

    for m in range(2):
        n_left, first, n_right = counts[m]

        @pl.when(n_left > 0)
        def _():
            load_left(m).wait()
            load_edge(0, m, m * per_rank + n_left - 1).wait()

            @pl.loop(0, n_left)
            def _(i):
                x = lbuf[m, pl.ds(pl.multiple_of(i * BLOCK, BLOCK), BLOCK), :].astype(jnp.float32)
                keep = edge[0, m].astype(jnp.float32)
                x = jnp.where(row + i * BLOCK < before[m], x, keep)
                packed[0, m, i] = x.astype(jnp.bfloat16)
                store(0, m, i, m * per_rank + i).start()

        @pl.when(n_right > 0)
        def _():
            load_right(m).wait()
            load_edge(1, m, m * per_rank + first).wait()
            wide[m, pl.ds(lead, quarter), :] = rbuf[m].astype(jnp.float32)
            skip = after[m] - first * BLOCK

            @pl.loop(0, n_right)
            def _(i):
                x = wide[m, pl.ds(lead + i * BLOCK - skip, BLOCK), :]
                keep = edge[1, m].astype(jnp.float32)
                x = jnp.where(row + i * BLOCK >= skip, x, keep)
                packed[1, m, i] = x.astype(jnp.bfloat16)
                store(1, m, i, m * per_rank + first + i).start()

    for m in range(2):
        n_left, first, n_right = counts[m]

        @pl.loop(0, n_left)
        def _(i):
            store(0, m, i, m * per_rank + i).wait()

        @pl.loop(0, n_right)
        def _(i):
            store(1, m, i, m * per_rank + first + i).wait()


def patch(outgoing, left, right, before, after, dest):
    quarter, width = left.shape[1:]
    most = quarter // BLOCK + 1
    dtype = outgoing.dtype
    return pl.pallas_call(
        functools.partial(patch_kernel, quarter),
        grid_spec=pltpu.PrefetchScalarGridSpec(
            num_scalar_prefetch=3,
            grid=(),
            in_specs=[pl.BlockSpec(memory_space=pl.ANY)] * 3,
            out_specs=pl.BlockSpec(memory_space=pl.ANY),
            scratch_shapes=[
                pltpu.VMEM((2, quarter, width), dtype),
                pltpu.VMEM((2, quarter, width), dtype),
                pltpu.VMEM((2, quarter + 2 * BLOCK, width), jnp.float32),
                pltpu.VMEM((2, 2, BLOCK, width), dtype),
                pltpu.VMEM((2, 2, most, BLOCK, width), dtype),
                pltpu.SemaphoreType.DMA((2, 2)),
                pltpu.SemaphoreType.DMA((2, 2)),
                pltpu.SemaphoreType.DMA((2, 2, most)),
            ],
        ),
        out_shape=jax.ShapeDtypeStruct(outgoing.shape, dtype),
        input_output_aliases={5: 0},
        cost_estimate=pl.CostEstimate(flops=0, bytes_accessed=6 << 20, transcendentals=0),
    )(before, after, dest, left, right, outgoing)


MESH = pl.DeviceIdType.MESH
Z = 4
Y = 4
X = 4


def exchange_order():
    offsets = list(itertools.product(range(Z), range(2), range(Y), range(X)))[1:]
    random.Random(0).shuffle(offsets)
    return sorted(offsets, key=lambda o: -sum(min(a, 4 - a) for a in (o[0], o[2], o[3])))


def exchange_kernel(order, outgoing, incoming, send_sem, recv_sem, own_sem):
    data = lax.axis_index("dp")
    tensor = lax.axis_index("tensor")
    me = data * (Y * X) + tensor
    z, core, y, x = data // 2, data % 2, tensor // X, tensor % X

    def peer(offset):
        dz, dc, dy, dx = offset
        return (((z + dz) % Z) * 2 + (core + dc) % 2, ((y + dy) % Y) * X + (x + dx) % X)

    barrier = pltpu.get_barrier_semaphore()
    for offset in order:
        pl.semaphore_signal(barrier, inc=1, device_id=peer(offset), device_id_type=MESH)
    own = pltpu.make_async_copy(outgoing.at[me], incoming.at[me], own_sem)
    own.start()
    count = len(order)
    pl.semaphore_wait(barrier, count)
    for offset in order:
        target = peer(offset)
        pltpu.make_async_remote_copy(
            src_ref=outgoing.at[target[0] * (Y * X) + target[1]],
            dst_ref=incoming.at[me],
            send_sem=send_sem,
            recv_sem=recv_sem,
            device_id=target,
            device_id_type=MESH,
        ).start()
    own.wait()
    sent, got = outgoing.at[pl.ds(0, count)], incoming.at[pl.ds(0, count)]
    pltpu.make_async_copy(got, got, recv_sem).wait()
    pltpu.make_async_copy(sent, sent, send_sem).wait()


def exchange(outgoing):
    return pl.pallas_call(
        functools.partial(exchange_kernel, exchange_order()),
        in_specs=[pl.BlockSpec(memory_space=pl.ANY)],
        out_specs=pl.BlockSpec(memory_space=pl.ANY),
        out_shape=jax.ShapeDtypeStruct(outgoing.shape, outgoing.dtype),
        scratch_shapes=[pltpu.SemaphoreType.DMA] * 3,
        compiler_params=pltpu.CompilerParams(collective_id=0, has_side_effects=True),
    )(outgoing)


PAIR = 2


def finish_kernel(source, *refs):
    pieces = refs[:PAIR]
    probe, stored, sketch = refs[PAIR:]
    n_data, height, width = pieces[0].shape
    for i in range(PAIR):
        for d in range(n_data):
            stored[i, :, d * width:(d + 1) * width] = pieces[i][d]
    x = stored[...].reshape(PAIR * height, n_data * width)
    y = jnp.dot(x, probe[...], preferred_element_type=jnp.float32)
    sketch[...] = y.reshape(sketch.shape)


def finish(incoming, probe, source):
    n_data, n_tensor, height, width = incoming.shape
    slots = source.shape[0]
    columns = n_data * width

    def piece(i):
        return pl.BlockSpec(
            (n_data, None, height, width), lambda g, source: (0, source[g * PAIR + i], 0, 0)
        )

    return pl.pallas_call(
        finish_kernel,
        grid_spec=pltpu.PrefetchScalarGridSpec(
            num_scalar_prefetch=1,
            grid=(slots // PAIR,),
            in_specs=[piece(i) for i in range(PAIR)]
            + [pl.BlockSpec(probe.shape, lambda g, source: (0, 0))],
            out_specs=[
                pl.BlockSpec((PAIR, height, columns), lambda g, source: (g, 0, 0)),
                pl.BlockSpec((PAIR, height, probe.shape[1]), lambda g, source: (g, 0, 0)),
            ],
        ),
        out_shape=[
            jax.ShapeDtypeStruct((slots, height, columns), incoming.dtype),
            jax.ShapeDtypeStruct((slots, height, probe.shape[1]), jnp.float32),
        ],
        cost_estimate=pl.CostEstimate(
            flops=2 * slots * height * columns * probe.shape[1],
            bytes_accessed=18 << 20,
            transcendentals=0,
        ),
    )(source, *([incoming] * PAIR), probe)


def shards(embed_rows, head_rows, row_offsets, slot_table, probe):
    n_tensor = lax.axis_size("tensor")
    n_data = lax.axis_size("dp")
    my_tensor = lax.axis_index("tensor")
    my_data = lax.axis_index("dp")
    quarter = R // 4
    height, width = embed_rows.shape
    buffers = [embed_rows, head_rows]
    own_start = row_offsets[:, my_tensor]
    next_start = row_offsets[:, my_tensor + 1]
    before = own_start - my_tensor * R
    after = next_start - my_tensor * R
    lead_part = jnp.stack([embed_rows[:quarter], head_rows[:quarter]])
    tail_begin = jnp.clip((my_tensor + 1) * R - own_start, 0, height - quarter)
    trail_part = jnp.stack(
        [lax.dynamic_slice_in_dim(buffers[m], tail_begin[m], quarter, 0) for m in range(2)]
    )
    from_right = from_behind(lead_part, "tensor", -1)
    from_left = from_behind(trail_part, "tensor", 1)

    devices = n_tensor * n_data
    per_rank = R // BLOCK
    total_blocks = per_rank * n_tensor
    slot_count = 2 * total_blocks // devices
    local = jnp.arange(2 * per_rank, dtype=jnp.int32)
    number = local // per_rank * total_blocks + my_tensor * per_rank + local % per_rank
    holder = jnp.arange(2 * total_blocks, dtype=jnp.int32) // slot_count
    dest = jnp.sum(jnp.where(slot_table[None, :] == number[:, None], holder[None, :], 0), axis=1)
    dest = dest.astype(jnp.int32)

    outgoing = pack_own(embed_rows, head_rows, before, dest, quarter)
    outgoing = patch(outgoing, from_left, from_right, before, after, dest)
    incoming = exchange(outgoing)
    writer = my_data * n_tensor + my_tensor
    mine = lax.dynamic_slice_in_dim(slot_table, writer * slot_count, slot_count)
    source = mine % total_blocks // per_rank
    incoming = incoming.reshape(n_data, n_tensor, BLOCK, width)
    stored, sketch = finish(incoming, probe, source)
    return (stored, sketch)


def solution(mesh):
    return jax.shard_map(
        shards,
        mesh=mesh,
        in_specs=(P("tensor", "dp"), P("tensor", "dp"), P(), P(), P()),
        out_specs=(P(("dp", "tensor"), None, None), P(("dp", "tensor"), None, None)),
        check_vma=False,
    )
```

```python
import functools
import itertools
import random

import jax
import jax.numpy as jnp
from jax import lax
from jax.experimental import pallas as pl
from jax.experimental.pallas import tpu as pltpu
from jax.sharding import PartitionSpec as P

R = 8192
BLOCK = 128
MESH = pl.DeviceIdType.MESH
Z = 4
Y = 4
X = 4
QUARTER = R // 4
LIFT = 16
TRAIL = QUARTER + LIFT
HIGH = R - QUARTER
PAD = BLOCK
OWN = PAD + R + QUARTER
FOREIGN = PAD + TRAIL
PACK = 8


def exchange_order():
    offsets = list(itertools.product(range(Z), range(2), range(Y), range(X)))[1:]
    random.Random(0).shuffle(offsets)
    offsets.sort(key=lambda o: -sum(min(a, 4 - a) for a in (o[0], o[2], o[3])))
    return offsets + [(0, 0, 0, 0)]


ORDER = exchange_order()


def save_kernel(
    offsets, picked, embed, head, incoming, low, high, own, arrived, foreign, trail, packed,
    load_sem, shift_send, shift_recv, send_sem, recv_sem, own_sem, plane_sem, space_sem,
):
    data = lax.axis_index("dp")
    tensor = lax.axis_index("tensor")
    me = data * (Y * X) + tensor
    z, core, y, x = data // 2, data % 2, tensor // X, tensor % X
    ranks = Y * X
    following = (data, (tensor + 1) % ranks)
    previous = (data, (tensor + ranks - 1) % ranks)

    def peer(offset):
        dz, dc, dy, dx = offset
        return (((z + dz) % Z) * 2 + (core + dc) % 2, ((y + dy) % Y) * X + (x + dx) % X)

    def signal(sem, device):
        pl.semaphore_signal(sem, inc=1, device_id=device, device_id_type=MESH)

    sources = (embed, head)
    height = embed.shape[0]

    def load(m, part):
        if part == 0:
            return pltpu.make_async_copy(
                sources[m].at[pl.ds(HIGH, height - HIGH)],
                high.at[pl.ds(m * (height - HIGH), height - HIGH)],
                load_sem.at[0, m],
            )
        return pltpu.make_async_copy(sources[m].at[pl.ds(0, HIGH)], low.at[m], load_sem.at[1, m])

    row = [(0, dc, 0, dx) for dc in range(2) for dx in range(X) if (dc, dx) != (0, 0)]
    column = [(0, 0, d, 0) for d in range(1, Y)]
    stack = [(d, 0, 0, 0) for d in range(1, Z)]
    barrier = pltpu.get_barrier_semaphore()
    signal(barrier, following)
    signal(barrier, previous)
    for offset in stack + column + row:
        signal(barrier, peer(offset))
    for part in range(2):
        for m in range(2):
            load(m, part).start()
    pl.semaphore_wait(barrier, 2 + len(stack + column + row))

    def lead(m):
        return pltpu.make_async_remote_copy(
            src_ref=sources[m].at[pl.ds(0, QUARTER)],
            dst_ref=arrived.at[m, 1, pl.ds(0, QUARTER)],
            send_sem=shift_send.at[1, m],
            recv_sem=shift_recv.at[1, m],
            device_id=previous,
            device_id_type=MESH,
        )

    def tail(m):
        return pltpu.make_async_remote_copy(
            src_ref=trail.at[m],
            dst_ref=arrived.at[m, 0],
            send_sem=shift_send.at[0, m],
            recv_sem=shift_recv.at[0, m],
            device_id=following,
            device_id_type=MESH,
        )

    lead(0).start()
    lead(1).start()
    load(0, 0).wait()
    load(1, 0).wait()
    for m in range(2):
        begin = (tensor + 1) * R - offsets[m, tensor] - HIGH
        begin = jnp.clip(begin, 0, height - HIGH - TRAIL + LIFT - 1)
        begin = lax.div(begin, LIFT) * LIFT
        begin = m * (height - HIGH) + begin
        trail[m] = high[pl.ds(begin, TRAIL), :]
    tail(0).start()
    tail(1).start()

    for offset in column:
        signal(plane_sem, peer(offset))
    pl.semaphore_wait(plane_sem, len(column))
    for offset in stack:
        signal(space_sem, peer(offset))
    load(0, 1).wait()
    load(1, 1).wait()
    step = 256
    for m in range(2):

        @pl.loop(0, HIGH // step)
        def _(i):
            at = pl.multiple_of(i * step, step)
            own[pl.ds(m * OWN + PAD + at, step), :] = low[m, pl.ds(at, step), :].astype(jnp.float32)

        @pl.loop(0, (R + QUARTER - HIGH) // step)
        def _(i):
            at = pl.multiple_of(i * step, step)
            rows = high[pl.ds(m * (height - HIGH) + at, step), :]
            own[pl.ds(m * OWN + PAD + HIGH + at, step), :] = rows.astype(jnp.float32)

    pl.semaphore_wait(space_sem, len(stack))

    for m in range(2):
        for side in range(2):
            (tail, lead)[side](m).wait_recv()

            @pl.loop(0, TRAIL // (3 * LIFT))
            def _(i):
                at = pl.multiple_of(i * 3 * LIFT, LIFT)
                rows = arrived[m, side, pl.ds(at, 3 * LIFT), :].astype(jnp.float32)
                foreign[pl.ds((m * 2 + side) * FOREIGN + PAD + at, 3 * LIFT), :] = rows

    earlier = (tensor + ranks - 1) % ranks
    befores = [offsets[m, tensor] - tensor * R for m in range(2)]
    afters = [offsets[m, tensor + 1] - tensor * R for m in range(2)]
    lifts = [lax.rem((earlier + 1) * R - offsets[m, earlier], LIFT) for m in range(2)]
    local_row = lax.broadcasted_iota(jnp.int32, (BLOCK, embed.shape[1]), 0)

    def pack(k):
        local = picked[k]
        m = lax.div(local, R // BLOCK)
        block = lax.rem(local, R // BLOCK)
        first = block * BLOCK
        before = befores[0] + m * (befores[1] - befores[0])
        after = afters[0] + m * (afters[1] - afters[0])
        lift = lifts[0] + m * (lifts[1] - lifts[0])
        own_at = m * OWN + PAD + jnp.clip(first - before, -PAD, R + QUARTER - BLOCK)
        left_at = jnp.clip(first + lift, -PAD, TRAIL - BLOCK)
        right_at = jnp.clip(first - after, -PAD, TRAIL - BLOCK)
        side = lax.div(block, R // BLOCK // 2)
        at = (m * 2 + side) * FOREIGN + PAD + left_at + side * (right_at - left_at)
        mine = own[pl.ds(own_at, BLOCK), :]
        theirs = foreign[pl.ds(at, BLOCK), :]
        keep = (local_row >= before - first) & (local_row < after - first)
        packed[k] = jnp.where(keep, mine, theirs).astype(packed.dtype)

    def send(k):
        return pltpu.make_async_remote_copy(
            src_ref=packed.at[k],
            dst_ref=incoming.at[me],
            send_sem=send_sem,
            recv_sem=recv_sem,
            device_id=peer(ORDER[k]),
            device_id_type=MESH,
        )

    count = len(ORDER)
    for group in range(0, count + PACK, PACK):
        if group < count:

            @pl.loop(group, group + PACK)
            def _(k):
                pack(k)

        for k in range(max(group - PACK, 0), min(group, count - 1)):
            send(k).start()
    own_copy = pltpu.make_async_copy(packed.at[count - 1], incoming.at[me], own_sem)
    own_copy.start()
    own_copy.wait()
    got, sent = incoming.at[pl.ds(0, count - 1)], packed.at[pl.ds(0, count - 1)]
    pltpu.make_async_copy(got, got, recv_sem).wait()
    pltpu.make_async_copy(sent, sent, send_sem).wait()
    for m in range(2):
        lead(m).wait_send()
        tail(m).wait_send()


def save(embed_rows, head_rows, row_offsets, picked):
    height, width = embed_rows.shape
    dtype = embed_rows.dtype
    return pl.pallas_call(
        save_kernel,
        grid_spec=pltpu.PrefetchScalarGridSpec(
            num_scalar_prefetch=2,
            grid=(),
            in_specs=[pl.BlockSpec(memory_space=pl.ANY)] * 2,
            out_specs=pl.BlockSpec(memory_space=pl.ANY),
            scratch_shapes=[
                pltpu.VMEM((2, HIGH, width), dtype),
                pltpu.VMEM((2 * (height - HIGH), width), dtype),
                pltpu.VMEM((2 * OWN, width), jnp.float32),
                pltpu.VMEM((2, 2, TRAIL, width), dtype),
                pltpu.VMEM((4 * FOREIGN, width), jnp.float32),
                pltpu.VMEM((2, TRAIL, width), dtype),
                pltpu.VMEM((len(ORDER), BLOCK, width), dtype),
                pltpu.SemaphoreType.DMA((2, 2)),
                pltpu.SemaphoreType.DMA((2, 2)),
                pltpu.SemaphoreType.DMA((2, 2)),
                pltpu.SemaphoreType.DMA,
                pltpu.SemaphoreType.DMA,
                pltpu.SemaphoreType.DMA,
                pltpu.SemaphoreType.REGULAR,
                pltpu.SemaphoreType.REGULAR,
            ],
        ),
        out_shape=jax.ShapeDtypeStruct((len(ORDER), BLOCK, width), dtype),
        compiler_params=pltpu.CompilerParams(collective_id=0, has_side_effects=True),
    )(row_offsets, picked, embed_rows, head_rows)


PAIR = 2


def finish_kernel(source, *refs):
    pieces = refs[:PAIR]
    probe, stored, sketch = refs[PAIR:]
    n_data, height, width = pieces[0].shape
    for i in range(PAIR):
        for d in range(n_data):
            stored[i, :, d * width:(d + 1) * width] = pieces[i][d]
    x = stored[...].reshape(PAIR * height, n_data * width)
    y = jnp.dot(x, probe[...], preferred_element_type=jnp.float32)
    sketch[...] = y.reshape(sketch.shape)


def finish(incoming, probe, source):
    n_data, n_tensor, height, width = incoming.shape
    slots = source.shape[0]
    columns = n_data * width

    def piece(i):
        return pl.BlockSpec(
            (n_data, None, height, width), lambda g, source: (0, source[g * PAIR + i], 0, 0)
        )

    return pl.pallas_call(
        finish_kernel,
        grid_spec=pltpu.PrefetchScalarGridSpec(
            num_scalar_prefetch=1,
            grid=(slots // PAIR,),
            in_specs=[piece(i) for i in range(PAIR)]
            + [pl.BlockSpec(probe.shape, lambda g, source: (0, 0))],
            out_specs=[
                pl.BlockSpec((PAIR, height, columns), lambda g, source: (g, 0, 0)),
                pl.BlockSpec((PAIR, height, probe.shape[1]), lambda g, source: (g, 0, 0)),
            ],
        ),
        out_shape=[
            jax.ShapeDtypeStruct((slots, height, columns), incoming.dtype),
            jax.ShapeDtypeStruct((slots, height, probe.shape[1]), jnp.float32),
        ],
        cost_estimate=pl.CostEstimate(
            flops=2 * slots * height * columns * probe.shape[1],
            bytes_accessed=18 << 20,
            transcendentals=0,
        ),
    )(source, *([incoming] * PAIR), probe)


def shards(embed_rows, head_rows, row_offsets, slot_table, probe):
    n_tensor = lax.axis_size("tensor")
    n_data = lax.axis_size("dp")
    tensor = lax.axis_index("tensor")
    data = lax.axis_index("dp")
    width = embed_rows.shape[1]
    per_rank = R // BLOCK
    total_blocks = per_rank * n_tensor
    slot_count = 2 * total_blocks // (n_tensor * n_data)

    dz, dc, dy, dx = (jnp.array(steps, jnp.int32) for steps in zip(*ORDER))
    target = ((data // 2 + dz) % Z * 2 + (data + dc) % 2) * n_tensor
    target = target + (tensor // X + dy) % Y * X + (tensor + dx) % X
    holder = jnp.arange(2 * total_blocks, dtype=jnp.int32) // slot_count
    local = jnp.where(
        slot_table % total_blocks // per_rank == tensor,
        slot_table // total_blocks * per_rank + slot_table % per_rank,
        0,
    )
    picked = jnp.sum(jnp.where(holder[None, :] == target[:, None], local[None, :], 0), axis=1)

    incoming = save(embed_rows, head_rows, row_offsets, picked.astype(jnp.int32))
    incoming = incoming.reshape(n_data, n_tensor, BLOCK, width)
    writer = data * n_tensor + tensor
    mine = lax.dynamic_slice_in_dim(slot_table, writer * slot_count, slot_count)
    source = mine % total_blocks // per_rank
    stored, sketch = finish(incoming, probe, source)
    return (stored, sketch)


def solution(mesh):
    return jax.shard_map(
        shards,
        mesh=mesh,
        in_specs=(P("tensor", "dp"), P("tensor", "dp"), P(), P(), P()),
        out_specs=(P(("dp", "tensor"), None, None), P(("dp", "tensor"), None, None)),
        check_vma=False,
    )
```

```python
import functools
import itertools
import random

import jax
import jax.numpy as jnp
from jax import lax
from jax.experimental import pallas as pl
from jax.experimental.pallas import tpu as pltpu
from jax.sharding import PartitionSpec as P

R = 8192
BLOCK = 128
MESH = pl.DeviceIdType.MESH
Z = 4
Y = 4
X = 4
QUARTER = R // 4
LIFT = 16
TRAIL = QUARTER + LIFT
HIGH = R - QUARTER
PAD = BLOCK
OWN = PAD + R + QUARTER
FOREIGN = PAD + TRAIL
PACK = 8


def exchange_order():
    offsets = list(itertools.product(range(Z), range(2), range(Y), range(X)))[1:]
    random.Random(0).shuffle(offsets)
    offsets.sort(key=lambda o: -sum(min(a, 4 - a) for a in (o[0], o[2], o[3])))
    return offsets + [(0, 0, 0, 0)]


ORDER = exchange_order()


def save_kernel(
    offsets, table, embed, head, incoming, lookup, picked, low, high, own, arrived, foreign, trail, packed,
    load_sem, shift_send, shift_recv, send_sem, recv_sem, plane_sem, space_sem,
):
    data = lax.axis_index("dp")
    tensor = lax.axis_index("tensor")
    me = data * (Y * X) + tensor
    z, core, y, x = data // 2, data % 2, tensor // X, tensor % X
    ranks = Y * X
    following = (data, (tensor + 1) % ranks)
    previous = (data, (tensor + ranks - 1) % ranks)

    def peer(offset):
        dz, dc, dy, dx = offset
        return (((z + dz) % Z) * 2 + (core + dc) % 2, ((y + dy) % Y) * X + (x + dx) % X)

    def signal(sem, device):
        pl.semaphore_signal(sem, inc=1, device_id=device, device_id_type=MESH)

    sources = (embed, head)
    height = embed.shape[0]

    def load(m, part):
        if part == 0:
            return pltpu.make_async_copy(
                sources[m].at[pl.ds(HIGH, height - HIGH)],
                high.at[pl.ds(m * (height - HIGH), height - HIGH)],
                load_sem.at[0, m],
            )
        return pltpu.make_async_copy(sources[m].at[pl.ds(0, HIGH)], low.at[m], load_sem.at[1, m])

    row = [(0, dc, 0, dx) for dc in range(2) for dx in range(X) if (dc, dx) != (0, 0)]
    column = [(0, 0, d, 0) for d in range(1, Y)]
    stack = [(d, 0, 0, 0) for d in range(1, Z)]
    barrier = pltpu.get_barrier_semaphore()
    signal(barrier, following)
    signal(barrier, previous)
    for offset in stack + column + row:
        signal(barrier, peer(offset))
    for part in range(2):
        for m in range(2):
            load(m, part).start()
    pl.semaphore_wait(barrier, 2 + len(stack + column + row))

    def lead(m):
        return pltpu.make_async_remote_copy(
            src_ref=sources[m].at[pl.ds(0, QUARTER)],
            dst_ref=arrived.at[m, 1, pl.ds(0, QUARTER)],
            send_sem=shift_send.at[1, m],
            recv_sem=shift_recv.at[1, m],
            device_id=previous,
            device_id_type=MESH,
        )

    def tail(m):
        return pltpu.make_async_remote_copy(
            src_ref=trail.at[m],
            dst_ref=arrived.at[m, 0],
            send_sem=shift_send.at[0, m],
            recv_sem=shift_recv.at[0, m],
            device_id=following,
            device_id_type=MESH,
        )

    lead(0).start()
    lead(1).start()
    load(0, 0).wait()
    load(1, 0).wait()
    for m in range(2):
        begin = (tensor + 1) * R - offsets[m, tensor] - HIGH
        begin = jnp.clip(begin, 0, height - HIGH - TRAIL + LIFT - 1)
        begin = lax.div(begin, LIFT) * LIFT
        begin = m * (height - HIGH) + begin
        trail[m] = high[pl.ds(begin, TRAIL), :]
    tail(0).start()
    tail(1).start()

    for offset in column:
        signal(plane_sem, peer(offset))
    pl.semaphore_wait(plane_sem, len(column))
    for offset in stack:
        signal(space_sem, peer(offset))
    per_rank = R // BLOCK
    slots = table.shape[0] // len(ORDER)

    @pl.loop(0, len(ORDER))
    def _(j):
        total = jnp.int32(0)
        for s in range(slots):
            number = table[j * slots + s]
            half = lax.div(number, per_rank * ranks)
            block = lax.rem(number, per_rank)
            rank = lax.rem(lax.div(number, per_rank), ranks)
            other = jnp.minimum(jnp.abs(rank - tensor), 1)
            total += (half * per_rank + block) * (1 - other)
        picked[j] = jnp.clip(total, 0, 2 * per_rank - 1)

    for k, offset in enumerate(ORDER):
        to = peer(offset)
        lookup[k] = to[0] * ranks + to[1]

    load(0, 1).wait()
    load(1, 1).wait()
    step = 256
    for m in range(2):

        @pl.loop(0, HIGH // step)
        def _(i):
            at = pl.multiple_of(i * step, step)
            own[pl.ds(m * OWN + PAD + at, step), :] = low[m, pl.ds(at, step), :].astype(jnp.float32)

        @pl.loop(0, (R + QUARTER - HIGH) // step)
        def _(i):
            at = pl.multiple_of(i * step, step)
            rows = high[pl.ds(m * (height - HIGH) + at, step), :]
            own[pl.ds(m * OWN + PAD + HIGH + at, step), :] = rows.astype(jnp.float32)

    pl.semaphore_wait(space_sem, len(stack))

    for m in range(2):
        for side in range(2):
            (tail, lead)[side](m).wait_recv()

            @pl.loop(0, TRAIL // (3 * LIFT))
            def _(i):
                at = pl.multiple_of(i * 3 * LIFT, LIFT)
                rows = arrived[m, side, pl.ds(at, 3 * LIFT), :].astype(jnp.float32)
                foreign[pl.ds((m * 2 + side) * FOREIGN + PAD + at, 3 * LIFT), :] = rows

    earlier = (tensor + ranks - 1) % ranks
    befores = [offsets[m, tensor] - tensor * R for m in range(2)]
    afters = [offsets[m, tensor + 1] - tensor * R for m in range(2)]
    lifts = [lax.rem((earlier + 1) * R - offsets[m, earlier], LIFT) for m in range(2)]
    local_row = lax.broadcasted_iota(jnp.int32, (BLOCK, embed.shape[1]), 0)

    def pack(k):
        local = picked[lookup[k]]
        m = lax.div(local, per_rank)
        block = lax.rem(local, per_rank)
        first = block * BLOCK
        before = befores[0] + m * (befores[1] - befores[0])
        after = afters[0] + m * (afters[1] - afters[0])
        lift = lifts[0] + m * (lifts[1] - lifts[0])
        own_at = m * OWN + PAD + jnp.clip(first - before, -PAD, R + QUARTER - BLOCK)
        left_at = jnp.clip(first + lift, -PAD, TRAIL - BLOCK)
        right_at = jnp.clip(first - after, -PAD, TRAIL - BLOCK)
        side = lax.div(block, per_rank // 2)
        at = (m * 2 + side) * FOREIGN + PAD + left_at + side * (right_at - left_at)
        mine = own[pl.ds(own_at, BLOCK), :]
        theirs = foreign[pl.ds(at, BLOCK), :]
        keep = (local_row >= before - first) & (local_row < after - first)
        packed[k] = jnp.where(keep, mine, theirs).astype(packed.dtype)

    def send(k):
        return pltpu.make_async_remote_copy(
            src_ref=packed.at[k],
            dst_ref=incoming.at[me],
            send_sem=send_sem,
            recv_sem=recv_sem,
            device_id=peer(ORDER[k]),
            device_id_type=MESH,
        )

    count = len(ORDER)
    for group in range(0, count + PACK, PACK):
        if group < count:

            @pl.loop(group, group + PACK)
            def _(k):
                pack(k)

        for k in range(max(group - PACK, 0), min(group, count - 1)):
            send(k).start()
    incoming[me] = packed[count - 1]
    everything = packed.at[pl.ds(0, count - 1)]
    pltpu.make_async_copy(everything, everything, recv_sem).wait()
    pltpu.make_async_copy(everything, everything, send_sem).wait()
    for m in range(2):
        lead(m).wait_send()
        tail(m).wait_send()


def save(embed_rows, head_rows, row_offsets, slot_table):
    height, width = embed_rows.shape
    dtype = embed_rows.dtype
    return pl.pallas_call(
        save_kernel,
        grid_spec=pltpu.PrefetchScalarGridSpec(
            num_scalar_prefetch=2,
            grid=(),
            in_specs=[pl.BlockSpec(memory_space=pl.ANY)] * 2,
            out_specs=pl.BlockSpec(memory_space=pltpu.VMEM),
            scratch_shapes=[
                pltpu.SMEM((len(ORDER),), jnp.int32),
                pltpu.SMEM((len(ORDER),), jnp.int32),
                pltpu.VMEM((2, HIGH, width), dtype),
                pltpu.VMEM((2 * (height - HIGH), width), dtype),
                pltpu.VMEM((2 * OWN, width), jnp.float32),
                pltpu.VMEM((2, 2, TRAIL, width), dtype),
                pltpu.VMEM((4 * FOREIGN, width), jnp.float32),
                pltpu.VMEM((2, TRAIL, width), dtype),
                pltpu.VMEM((len(ORDER), BLOCK, width), dtype),
                pltpu.SemaphoreType.DMA((2, 2)),
                pltpu.SemaphoreType.DMA((2, 2)),
                pltpu.SemaphoreType.DMA((2, 2)),
                pltpu.SemaphoreType.DMA,
                pltpu.SemaphoreType.DMA,
                pltpu.SemaphoreType.REGULAR,
                pltpu.SemaphoreType.REGULAR,
            ],
        ),
        out_shape=pltpu.VMEM((len(ORDER), BLOCK, width), dtype),
        compiler_params=pltpu.CompilerParams(
            collective_id=0, has_side_effects=True, vmem_limit_bytes=34 << 20
        ),
    )(row_offsets, slot_table, embed_rows, head_rows)


TAKE = 2
BUFFERS = 4


def finish_kernel(table, incoming, weights, stored, sketch, gathered, product, stored_sem, sketch_sem):
    n_data, n_tensor, height, width = incoming.shape
    slots = stored.shape[0]
    per_rank = R // BLOCK
    writer = lax.axis_index("dp") * n_tensor + lax.axis_index("tensor")
    rows = TAKE * height

    def put_stored(g):
        return pltpu.make_async_copy(
            gathered.at[pl.ds(g * TAKE, TAKE)], stored.at[pl.ds(g * TAKE, TAKE)], stored_sem.at[g]
        )

    def put_sketch(g):
        return pltpu.make_async_copy(
            product.at[g % BUFFERS], sketch.at[pl.ds(g * rows, rows)], sketch_sem.at[g]
        )

    groups = slots // TAKE
    for g in range(groups):
        for i in range(TAKE):
            slot = g * TAKE + i
            rank = lax.rem(lax.div(table[writer * slots + slot], per_rank), n_tensor)
            for d in range(n_data):
                gathered[slot, :, d * width:(d + 1) * width] = incoming[d, rank]
        put_stored(g).start()
        if g >= BUFFERS:
            put_sketch(g - BUFFERS).wait()
        x = gathered[g * TAKE:(g + 1) * TAKE].reshape(rows, n_data * width)
        product[g % BUFFERS] = jnp.dot(x, weights[...], preferred_element_type=jnp.float32)
        put_sketch(g).start()
    for g in range(groups):
        put_stored(g).wait()
    for g in range(groups - BUFFERS, groups):
        put_sketch(g).wait()


def finish(incoming, probe, slot_table):
    n_data, n_tensor, height, width = incoming.shape
    slots = slot_table.shape[0] // (n_data * n_tensor)
    columns = n_data * width
    stored, sketch = pl.pallas_call(
        finish_kernel,
        grid_spec=pltpu.PrefetchScalarGridSpec(
            num_scalar_prefetch=1,
            grid=(),
            in_specs=[pl.BlockSpec(memory_space=pltpu.VMEM)] * 2,
            out_specs=[pl.BlockSpec(memory_space=pl.ANY)] * 2,
            scratch_shapes=[
                pltpu.VMEM((slots, height, columns), incoming.dtype),
                pltpu.VMEM((BUFFERS, TAKE * height, probe.shape[1]), jnp.float32),
                pltpu.SemaphoreType.DMA((slots // TAKE,)),
                pltpu.SemaphoreType.DMA((slots // TAKE,)),
            ],
        ),
        out_shape=[
            jax.ShapeDtypeStruct((slots, height, columns), incoming.dtype),
            jax.ShapeDtypeStruct((slots * height, probe.shape[1]), jnp.float32),
        ],
        compiler_params=pltpu.CompilerParams(vmem_limit_bytes=20 << 20),
    )(slot_table, incoming, probe)
    return stored, sketch.reshape(slots, height, probe.shape[1])


def shards(embed_rows, head_rows, row_offsets, slot_table, probe):
    n_tensor = lax.axis_size("tensor")
    n_data = lax.axis_size("dp")
    probe = pltpu.with_memory_space_constraint(probe, pltpu.VMEM)
    embed_rows, head_rows, row_offsets, slot_table = (
        pltpu.with_memory_space_constraint(a, pltpu.HBM)
        for a in (embed_rows, head_rows, row_offsets, slot_table)
    )
    incoming = save(embed_rows, head_rows, row_offsets, slot_table)
    incoming = incoming.reshape(n_data, n_tensor, BLOCK, embed_rows.shape[1])
    stored, sketch = finish(incoming, probe, slot_table)
    return (stored, sketch)


def solution(mesh):
    return jax.shard_map(
        shards,
        mesh=mesh,
        in_specs=(P("tensor", "dp"), P("tensor", "dp"), P(), P(), P()),
        out_specs=(P(("dp", "tensor"), None, None), P(("dp", "tensor"), None, None)),
        check_vma=False,
    )
```

```python
import functools
import itertools
import random

import jax
import jax.numpy as jnp
from jax import lax
from jax.experimental import pallas as pl
from jax.experimental.pallas import tpu as pltpu
from jax.sharding import PartitionSpec as P

R = 8192
BLOCK = 128
MESH = pl.DeviceIdType.MESH
Z = 4
Y = 4
X = 4
QUARTER = R // 4
LIFT = 16
TRAIL = QUARTER + LIFT
HIGH = R - QUARTER
PAD = BLOCK
OWN = PAD + R + QUARTER
FOREIGN = PAD + TRAIL
STEP = 3 * LIFT
UNROLL = 4
PIECES = ((0, 0, TRAIL), (1, 0, 32 * STEP), (1, 32 * STEP, 11 * STEP))
ROUNDS = (0, 4, 8) + tuple(range(16, 129, 8))


def exchange_order():
    offsets = list(itertools.product(range(Z), range(2), range(Y), range(X)))[1:]
    random.Random(0).shuffle(offsets)
    offsets.sort(key=lambda o: -sum(min(a, 4 - a) for a in (o[0], o[2], o[3])))
    return offsets + [(0, 0, 0, 0)]


ORDER = exchange_order()


def save_kernel(
    offsets_hbm, table_hbm, embed, head, gathered, offsets, table, incoming, lookup, picked, low, high, own, arrived, foreign, trail, packed,
    load_sem, shift_send, shift_recv, scalar_sem, send_sem, recv_sem, plane_sem, space_sem,
):
    data = lax.axis_index("dp")
    tensor = lax.axis_index("tensor")
    me = data * (Y * X) + tensor
    z, core, y, x = data // 2, data % 2, tensor // X, tensor % X
    ranks = Y * X
    following = (data, (tensor + 1) % ranks)
    previous = (data, (tensor + ranks - 1) % ranks)

    def peer(offset):
        dz, dc, dy, dx = offset
        return (((z + dz) % Z) * 2 + (core + dc) % 2, ((y + dy) % Y) * X + (x + dx) % X)

    def signal(sem, device):
        pl.semaphore_signal(sem, inc=1, device_id=device, device_id_type=MESH)

    sources = (embed, head)
    height = embed.shape[0]

    def load(m, part):
        if part == 0:
            return pltpu.make_async_copy(
                sources[m].at[pl.ds(HIGH, height - HIGH)],
                high.at[pl.ds(m * (height - HIGH), height - HIGH)],
                load_sem.at[0, m],
            )
        return pltpu.make_async_copy(sources[m].at[pl.ds(0, HIGH)], low.at[m], load_sem.at[1, m])

    row = [(0, dc, 0, dx) for dc in range(2) for dx in range(X) if (dc, dx) != (0, 0)]
    column = [(0, 0, d, 0) for d in range(1, Y)]
    stack = [(d, 0, 0, 0) for d in range(1, Z)]
    barrier = pltpu.get_barrier_semaphore()
    signal(barrier, following)
    signal(barrier, previous)
    for offset in stack + column + row:
        signal(barrier, peer(offset))
    scalars = [
        pltpu.make_async_copy(offsets_hbm, offsets, scalar_sem.at[0]),
        pltpu.make_async_copy(table_hbm, table, scalar_sem.at[1]),
    ]
    for copy in scalars:
        copy.start()
    for part in range(2):
        for m in range(2):
            load(m, part).start()
    pl.semaphore_wait(barrier, 2 + len(stack + column + row))

    def shift(side, piece):
        m, first, rows = PIECES[piece]
        if side == 0:
            source = trail.at[m, pl.ds(first, rows)]
        else:
            rows = min(rows, QUARTER - first)
            source = sources[m].at[pl.ds(first, rows)]
        return pltpu.make_async_remote_copy(
            src_ref=source,
            dst_ref=arrived.at[m, side, pl.ds(first, rows)],
            send_sem=shift_send.at[side, piece],
            recv_sem=shift_recv.at[side, piece],
            device_id=(following, previous)[side],
            device_id_type=MESH,
        )

    for piece in range(len(PIECES)):
        shift(1, piece).start()
    for copy in scalars:
        copy.wait()
    load(0, 0).wait()
    load(1, 0).wait()
    for m in range(2):
        begin = (tensor + 1) * R - offsets[m, tensor] - HIGH
        begin = jnp.clip(begin, 0, height - HIGH - TRAIL + LIFT - 1)
        begin = lax.div(begin, LIFT) * LIFT
        begin = m * (height - HIGH) + begin
        trail[m] = high[pl.ds(begin, TRAIL), :]
    for piece in range(len(PIECES)):
        shift(0, piece).start()

    for offset in column:
        signal(plane_sem, peer(offset))
    pl.semaphore_wait(plane_sem, len(column))
    for offset in stack:
        signal(space_sem, peer(offset))
    per_rank = R // BLOCK
    slots = table.shape[0] // len(ORDER)

    @pl.loop(0, len(ORDER))
    def _(j):
        total = jnp.int32(0)
        for s in range(slots):
            number = table[j * slots + s]
            half = lax.div(number, per_rank * ranks)
            block = lax.rem(number, per_rank)
            rank = lax.rem(lax.div(number, per_rank), ranks)
            other = jnp.minimum(jnp.abs(rank - tensor), 1)
            total += (half * per_rank + block) * (1 - other)
        picked[j] = jnp.clip(total, 0, 2 * per_rank - 1)

    for k, offset in enumerate(ORDER):
        to = peer(offset)
        lookup[k] = to[0] * ranks + to[1]

    load(0, 1).wait()
    load(1, 1).wait()
    step = 256
    for m in range(2):

        @pl.loop(0, HIGH // step)
        def _(i):
            at = pl.multiple_of(i * step, step)
            own[pl.ds(m * OWN + PAD + at, step), :] = low[m, pl.ds(at, step), :].astype(jnp.float32)

        @pl.loop(0, (R + QUARTER - HIGH) // step)
        def _(i):
            at = pl.multiple_of(i * step, step)
            rows = high[pl.ds(m * (height - HIGH) + at, step), :]
            own[pl.ds(m * OWN + PAD + HIGH + at, step), :] = rows.astype(jnp.float32)

    pl.semaphore_wait(space_sem, len(stack))

    for piece, (m, first_row, rows) in enumerate(PIECES):
        for side in range(2):
            shift(side, piece).wait_recv()

            @pl.loop(0, rows // STEP)
            def _(i):
                at = pl.multiple_of(first_row + i * STEP, LIFT)
                rows = arrived[m, side, pl.ds(at, STEP), :].astype(jnp.float32)
                foreign[pl.ds((m * 2 + side) * FOREIGN + PAD + at, STEP), :] = rows

    earlier = (tensor + ranks - 1) % ranks
    befores = [offsets[m, tensor] - tensor * R for m in range(2)]
    afters = [offsets[m, tensor + 1] - tensor * R for m in range(2)]
    lifts = [lax.rem((earlier + 1) * R - offsets[m, earlier], LIFT) for m in range(2)]
    local_row = lax.broadcasted_iota(jnp.int32, (BLOCK, embed.shape[1]), 0)

    def pack(k):
        local = picked[lookup[k]]
        m = lax.div(local, per_rank)
        block = lax.rem(local, per_rank)
        first = block * BLOCK
        before = befores[0] + m * (befores[1] - befores[0])
        after = afters[0] + m * (afters[1] - afters[0])
        lift = lifts[0] + m * (lifts[1] - lifts[0])
        own_at = m * OWN + PAD + jnp.clip(first - before, -PAD, R + QUARTER - BLOCK)
        left_at = jnp.clip(first + lift, -PAD, TRAIL - BLOCK)
        right_at = jnp.clip(first - after, -PAD, TRAIL - BLOCK)
        side = lax.div(block, per_rank // 2)
        at = (m * 2 + side) * FOREIGN + PAD + left_at + side * (right_at - left_at)
        mine = own[pl.ds(own_at, BLOCK), :]
        theirs = foreign[pl.ds(at, BLOCK), :]
        keep = (local_row >= before - first) & (local_row < after - first)
        packed[k] = jnp.where(keep, mine, theirs).astype(packed.dtype)

    def send(k):
        return pltpu.make_async_remote_copy(
            src_ref=packed.at[k],
            dst_ref=incoming.at[me],
            send_sem=send_sem,
            recv_sem=recv_sem,
            device_id=peer(ORDER[k]),
            device_id_type=MESH,
        )

    count = len(ORDER)
    for start, stop, behind in zip(ROUNDS, ROUNDS[1:] + (count,), (0,) + ROUNDS):
        if start < stop:

            @pl.loop(start, stop, unroll=UNROLL)
            def _(k):
                pack(k)

        for k in range(behind, min(start, count - 1)):
            send(k).start()
    incoming[me] = packed[count - 1]
    everything = packed.at[pl.ds(0, count - 1)]
    pltpu.make_async_copy(everything, everything, recv_sem).wait()
    width = embed.shape[1]

    @pl.loop(0, slots, unroll=2)
    def _(slot):
        rank = lax.rem(lax.div(table[me * slots + slot], per_rank), ranks)
        at = pl.ds(pl.multiple_of(slot * BLOCK, BLOCK), BLOCK)
        for d in range(2 * Z):
            gathered[at, d * width:(d + 1) * width] = incoming[d * ranks + rank]

    pltpu.make_async_copy(everything, everything, send_sem).wait()
    for piece in range(len(PIECES)):
        for side in range(2):
            shift(side, piece).wait_send()


def save(embed_rows, head_rows, row_offsets, slot_table):
    height, width = embed_rows.shape
    dtype = embed_rows.dtype
    slots = slot_table.shape[0] // len(ORDER)
    return pl.pallas_call(
        save_kernel,
        in_specs=[pl.BlockSpec(memory_space=pl.ANY)] * 4,
        out_specs=pl.BlockSpec(memory_space=pltpu.VMEM),
        scratch_shapes=[
            pltpu.SMEM(row_offsets.shape, jnp.int32),
            pltpu.SMEM(slot_table.shape, jnp.int32),
            pltpu.VMEM((len(ORDER), BLOCK, width), dtype),
            pltpu.SMEM((len(ORDER),), jnp.int32),
            pltpu.SMEM((len(ORDER),), jnp.int32),
            pltpu.VMEM((2, HIGH, width), dtype),
            pltpu.VMEM((2 * (height - HIGH), width), dtype),
            pltpu.VMEM((2 * OWN, width), jnp.float32),
            pltpu.VMEM((2, 2, TRAIL, width), dtype),
            pltpu.VMEM((4 * FOREIGN, width), jnp.float32),
            pltpu.VMEM((2, TRAIL, width), dtype),
            pltpu.VMEM((len(ORDER), BLOCK, width), dtype),
            pltpu.SemaphoreType.DMA((2, 2)),
            pltpu.SemaphoreType.DMA((2, len(PIECES))),
            pltpu.SemaphoreType.DMA((2, len(PIECES))),
            pltpu.SemaphoreType.DMA((2,)),
            pltpu.SemaphoreType.DMA,
            pltpu.SemaphoreType.DMA,
            pltpu.SemaphoreType.REGULAR,
            pltpu.SemaphoreType.REGULAR,
        ],
        out_shape=pltpu.VMEM((slots * BLOCK, 2 * Z * width), dtype),
        compiler_params=pltpu.CompilerParams(
            collective_id=0, has_side_effects=True, vmem_limit_bytes=38 << 20
        ),
    )(row_offsets, slot_table, embed_rows, head_rows)


ROWS = 256
BUFFERS = 4


def finish_kernel(gathered, weights, stored, sketch, product, stored_sem, sketch_sem):
    groups = gathered.shape[0] // ROWS

    def put_stored(g):
        at = pl.ds(g * ROWS, ROWS)
        return pltpu.make_async_copy(gathered.at[at], stored.at[at], stored_sem.at[g])

    def put_sketch(g):
        return pltpu.make_async_copy(
            product.at[g % BUFFERS], sketch.at[pl.ds(g * ROWS, ROWS)], sketch_sem.at[g]
        )

    for g in range(groups):
        put_stored(g).start()
    for g in range(groups):
        if g >= BUFFERS:
            put_sketch(g - BUFFERS).wait()
        x = gathered[g * ROWS:(g + 1) * ROWS]
        product[g % BUFFERS] = jnp.dot(x, weights[...], preferred_element_type=jnp.float32)
        put_sketch(g).start()
    for g in range(groups):
        put_stored(g).wait()
    for g in range(groups - BUFFERS, groups):
        put_sketch(g).wait()


def finish(gathered, probe):
    rows, columns = gathered.shape
    return pl.pallas_call(
        finish_kernel,
        in_specs=[pl.BlockSpec(memory_space=pltpu.VMEM)] * 2,
        out_specs=[pl.BlockSpec(memory_space=pl.ANY)] * 2,
        scratch_shapes=[
            pltpu.VMEM((BUFFERS, ROWS, probe.shape[1]), jnp.float32),
            pltpu.SemaphoreType.DMA((rows // ROWS,)),
            pltpu.SemaphoreType.DMA((rows // ROWS,)),
        ],
        out_shape=[
            jax.ShapeDtypeStruct((rows, columns), gathered.dtype),
            jax.ShapeDtypeStruct((rows, probe.shape[1]), jnp.float32),
        ],
        compiler_params=pltpu.CompilerParams(vmem_limit_bytes=20 << 20),
    )(gathered, probe)


def shards(embed_rows, head_rows, row_offsets, slot_table, probe):
    probe = pltpu.with_memory_space_constraint(probe, pltpu.VMEM)
    embed_rows, head_rows, row_offsets, slot_table = (
        pltpu.with_memory_space_constraint(a, pltpu.HBM)
        for a in (embed_rows, head_rows, row_offsets, slot_table)
    )
    gathered = save(embed_rows, head_rows, row_offsets, slot_table)
    stored, sketch = finish(gathered, probe)
    return (stored.reshape(-1, BLOCK, stored.shape[1]), sketch.reshape(-1, BLOCK, sketch.shape[1]))


def solution(mesh):
    return jax.shard_map(
        shards,
        mesh=mesh,
        in_specs=(P("tensor", "dp"), P("tensor", "dp"), P(), P(), P()),
        out_specs=(P(("dp", "tensor"), None, None), P(("dp", "tensor"), None, None)),
        check_vma=False,
    )
```

```python
import functools
import itertools
import random

import jax
import jax.numpy as jnp
from jax import lax
from jax.experimental import pallas as pl
from jax.experimental.pallas import tpu as pltpu
from jax.sharding import PartitionSpec as P

R = 8192
BLOCK = 128
MESH = pl.DeviceIdType.MESH
Z = 4
Y = 4
X = 4
QUARTER = R // 4
LIFT = 16
TRAIL = QUARTER + LIFT
HIGH = R - QUARTER
PAD = BLOCK
OWN = PAD + R + QUARTER
FOREIGN = PAD + TRAIL
STEP = 3 * LIFT
UNROLL = 4
PIECES = ((0, 0, TRAIL), (1, 0, 32 * STEP), (1, 32 * STEP, 11 * STEP))
ROUNDS = (0, 4, 8) + tuple(range(16, 129, 8))


def exchange_order():
    offsets = list(itertools.product(range(Z), range(2), range(Y), range(X)))[1:]
    random.Random(0).shuffle(offsets)
    offsets.sort(key=lambda o: -sum(min(a, 4 - a) for a in (o[0], o[2], o[3])))
    return offsets + [(0, 0, 0, 0)]


ORDER = exchange_order()


def save_kernel(
    offsets_hbm, table_hbm, embed, head, gathered, offsets, table, incoming, lookup, picked, low, high_embed, high_head, own, arrived, foreign, trail, packed,
    load_sem, shift_send, shift_recv, scalar_sem, send_sem, recv_sem, plane_sem, space_sem,
):
    data = lax.axis_index("dp")
    tensor = lax.axis_index("tensor")
    me = data * (Y * X) + tensor
    z, core, y, x = data // 2, data % 2, tensor // X, tensor % X
    ranks = Y * X
    following = (data, (tensor + 1) % ranks)
    previous = (data, (tensor + ranks - 1) % ranks)

    def peer(offset):
        dz, dc, dy, dx = offset
        return (((z + dz) % Z) * 2 + (core + dc) % 2, ((y + dy) % Y) * X + (x + dx) % X)

    def signal(sem, device):
        pl.semaphore_signal(sem, inc=1, device_id=device, device_id_type=MESH)

    sources = (embed, head)
    high = (high_embed, high_head)
    height = embed.shape[0]

    def load(m, part):
        if part == 0:
            return pltpu.make_async_copy(
                sources[m].at[pl.ds(HIGH, height - HIGH)],
                high[m],
                load_sem.at[0, m],
            )
        return pltpu.make_async_copy(sources[m].at[pl.ds(0, HIGH)], low.at[m], load_sem.at[1, m])

    row = [(0, dc, 0, dx) for dc in range(2) for dx in range(X) if (dc, dx) != (0, 0)]
    column = [(0, 0, d, 0) for d in range(1, Y)]
    stack = [(d, 0, 0, 0) for d in range(1, Z)]
    barrier = pltpu.get_barrier_semaphore()
    signal(barrier, following)
    signal(barrier, previous)
    for offset in stack + column + row:
        signal(barrier, peer(offset))
    scalars = [
        pltpu.make_async_copy(offsets_hbm, offsets, scalar_sem.at[0]),
        pltpu.make_async_copy(table_hbm, table, scalar_sem.at[1]),
    ]
    for copy in scalars:
        copy.start()
    load(0, 0).start()
    load(1, 0).start()
    pl.semaphore_wait(barrier, 2 + len(stack + column + row))

    def shift(side, piece):
        m, first, rows = PIECES[piece]
        if side == 0:
            source = trail.at[m, pl.ds(first, rows)]
        else:
            rows = min(rows, QUARTER - first)
            source = sources[m].at[pl.ds(first, rows)]
        return pltpu.make_async_remote_copy(
            src_ref=source,
            dst_ref=arrived.at[m, side, pl.ds(first, rows)],
            send_sem=shift_send.at[side, piece],
            recv_sem=shift_recv.at[side, piece],
            device_id=(following, previous)[side],
            device_id_type=MESH,
        )

    for piece in range(len(PIECES)):
        shift(1, piece).start()
    scalars[0].wait()
    for m in range(2):
        load(m, 0).wait()
        begin = (tensor + 1) * R - offsets[m, tensor] - HIGH
        begin = jnp.clip(begin, 0, height - HIGH - TRAIL + LIFT - 1)
        begin = lax.div(begin, LIFT) * LIFT
        trail[m] = high[m][pl.ds(begin, TRAIL), :]
        load(m, 1).start()
        for piece in range(len(PIECES)):
            if PIECES[piece][0] == m:
                shift(0, piece).start()
    scalars[1].wait()

    for offset in column:
        signal(plane_sem, peer(offset))
    pl.semaphore_wait(plane_sem, len(column))
    for offset in stack:
        signal(space_sem, peer(offset))
    per_rank = R // BLOCK
    slots = table.shape[0] // len(ORDER)

    @pl.loop(0, len(ORDER))
    def _(j):
        total = jnp.int32(0)
        for s in range(slots):
            number = table[j * slots + s]
            half = lax.div(number, per_rank * ranks)
            block = lax.rem(number, per_rank)
            rank = lax.rem(lax.div(number, per_rank), ranks)
            other = jnp.minimum(jnp.abs(rank - tensor), 1)
            total += (half * per_rank + block) * (1 - other)
        picked[j] = jnp.clip(total, 0, 2 * per_rank - 1)

    for k, offset in enumerate(ORDER):
        to = peer(offset)
        lookup[k] = to[0] * ranks + to[1]

    load(0, 1).wait()
    load(1, 1).wait()
    step = 256
    for m in range(2):

        @pl.loop(0, HIGH // step)
        def _(i):
            at = pl.multiple_of(i * step, step)
            own[pl.ds(m * OWN + PAD + at, step), :] = low[m, pl.ds(at, step), :].astype(jnp.float32)

        @pl.loop(0, (R + QUARTER - HIGH) // step)
        def _(i):
            at = pl.multiple_of(i * step, step)
            rows = high[m][pl.ds(at, step), :]
            own[pl.ds(m * OWN + PAD + HIGH + at, step), :] = rows.astype(jnp.float32)

    pl.semaphore_wait(space_sem, len(stack))

    for piece, (m, first_row, rows) in enumerate(PIECES):
        for side in range(2):
            shift(side, piece).wait_recv()

            @pl.loop(0, rows // STEP)
            def _(i):
                at = pl.multiple_of(first_row + i * STEP, LIFT)
                rows = arrived[m, side, pl.ds(at, STEP), :].astype(jnp.float32)
                foreign[pl.ds((m * 2 + side) * FOREIGN + PAD + at, STEP), :] = rows

    earlier = (tensor + ranks - 1) % ranks
    befores = [offsets[m, tensor] - tensor * R for m in range(2)]
    afters = [offsets[m, tensor + 1] - tensor * R for m in range(2)]
    lifts = [lax.rem((earlier + 1) * R - offsets[m, earlier], LIFT) for m in range(2)]
    local_row = lax.broadcasted_iota(jnp.int32, (BLOCK, embed.shape[1]), 0)

    def pack(k):
        local = picked[lookup[k]]
        m = lax.div(local, per_rank)
        block = lax.rem(local, per_rank)
        first = block * BLOCK
        before = befores[0] + m * (befores[1] - befores[0])
        after = afters[0] + m * (afters[1] - afters[0])
        lift = lifts[0] + m * (lifts[1] - lifts[0])
        own_at = m * OWN + PAD + jnp.clip(first - before, -PAD, R + QUARTER - BLOCK)
        left_at = jnp.clip(first + lift, -PAD, TRAIL - BLOCK)
        right_at = jnp.clip(first - after, -PAD, TRAIL - BLOCK)
        side = lax.div(block, per_rank // 2)
        at = (m * 2 + side) * FOREIGN + PAD + left_at + side * (right_at - left_at)
        mine = own[pl.ds(own_at, BLOCK), :]
        theirs = foreign[pl.ds(at, BLOCK), :]
        keep = (local_row >= before - first) & (local_row < after - first)
        packed[k] = jnp.where(keep, mine, theirs).astype(packed.dtype)

    def send(k):
        return pltpu.make_async_remote_copy(
            src_ref=packed.at[k],
            dst_ref=incoming.at[me],
            send_sem=send_sem,
            recv_sem=recv_sem,
            device_id=peer(ORDER[k]),
            device_id_type=MESH,
        )

    count = len(ORDER)
    for start, stop, behind in zip(ROUNDS, ROUNDS[1:] + (count,), (0,) + ROUNDS):
        if start < stop:

            @pl.loop(start, stop, unroll=UNROLL)
            def _(k):
                pack(k)

        for k in range(behind, min(start, count - 1)):
            send(k).start()
    incoming[me] = packed[count - 1]
    everything = packed.at[pl.ds(0, count - 1)]
    pltpu.make_async_copy(everything, everything, recv_sem).wait()
    width = embed.shape[1]

    @pl.loop(0, slots, unroll=2)
    def _(slot):
        rank = lax.rem(lax.div(table[me * slots + slot], per_rank), ranks)
        at = pl.ds(pl.multiple_of(slot * BLOCK, BLOCK), BLOCK)
        for d in range(2 * Z):
            gathered[at, d * width:(d + 1) * width] = incoming[d * ranks + rank]

    pltpu.make_async_copy(everything, everything, send_sem).wait()
    for piece in range(len(PIECES)):
        for side in range(2):
            shift(side, piece).wait_send()


def save(embed_rows, head_rows, row_offsets, slot_table):
    height, width = embed_rows.shape
    dtype = embed_rows.dtype
    slots = slot_table.shape[0] // len(ORDER)
    return pl.pallas_call(
        save_kernel,
        in_specs=[pl.BlockSpec(memory_space=pl.ANY)] * 4,
        out_specs=pl.BlockSpec(memory_space=pltpu.VMEM),
        scratch_shapes=[
            pltpu.SMEM(row_offsets.shape, jnp.int32),
            pltpu.SMEM(slot_table.shape, jnp.int32),
            pltpu.VMEM((len(ORDER), BLOCK, width), dtype),
            pltpu.SMEM((len(ORDER),), jnp.int32),
            pltpu.SMEM((len(ORDER),), jnp.int32),
            pltpu.VMEM((2, HIGH, width), dtype),
            pltpu.VMEM((height - HIGH, width), dtype),
            pltpu.VMEM((height - HIGH, width), dtype),
            pltpu.VMEM((2 * OWN, width), jnp.float32),
            pltpu.VMEM((2, 2, TRAIL, width), dtype),
            pltpu.VMEM((4 * FOREIGN, width), jnp.float32),
            pltpu.VMEM((2, TRAIL, width), dtype),
            pltpu.VMEM((len(ORDER), BLOCK, width), dtype),
            pltpu.SemaphoreType.DMA((2, 2)),
            pltpu.SemaphoreType.DMA((2, len(PIECES))),
            pltpu.SemaphoreType.DMA((2, len(PIECES))),
            pltpu.SemaphoreType.DMA((2,)),
            pltpu.SemaphoreType.DMA,
            pltpu.SemaphoreType.DMA,
            pltpu.SemaphoreType.REGULAR,
            pltpu.SemaphoreType.REGULAR,
        ],
        out_shape=pltpu.VMEM((slots * BLOCK, 2 * Z * width), dtype),
        compiler_params=pltpu.CompilerParams(
            collective_id=0, has_side_effects=True, vmem_limit_bytes=38 << 20
        ),
    )(row_offsets, slot_table, embed_rows, head_rows)


ROWS = 256
BUFFERS = 4


def finish_kernel(gathered, weights, stored, sketch, product, stored_sem, sketch_sem):
    groups = gathered.shape[0] // ROWS

    def put_stored(g):
        at = pl.ds(g * ROWS, ROWS)
        return pltpu.make_async_copy(gathered.at[at], stored.at[at], stored_sem.at[g])

    def put_sketch(g):
        return pltpu.make_async_copy(
            product.at[g % BUFFERS], sketch.at[pl.ds(g * ROWS, ROWS)], sketch_sem.at[g]
        )

    for g in range(groups):
        put_stored(g).start()
    for g in range(groups):
        if g >= BUFFERS:
            put_sketch(g - BUFFERS).wait()
        x = gathered[g * ROWS:(g + 1) * ROWS]
        product[g % BUFFERS] = jnp.dot(x, weights[...], preferred_element_type=jnp.float32)
        put_sketch(g).start()
    for g in range(groups):
        put_stored(g).wait()
    for g in range(groups - BUFFERS, groups):
        put_sketch(g).wait()


def finish(gathered, probe):
    rows, columns = gathered.shape
    return pl.pallas_call(
        finish_kernel,
        in_specs=[pl.BlockSpec(memory_space=pltpu.VMEM)] * 2,
        out_specs=[pl.BlockSpec(memory_space=pl.ANY)] * 2,
        scratch_shapes=[
            pltpu.VMEM((BUFFERS, ROWS, probe.shape[1]), jnp.float32),
            pltpu.SemaphoreType.DMA((rows // ROWS,)),
            pltpu.SemaphoreType.DMA((rows // ROWS,)),
        ],
        out_shape=[
            jax.ShapeDtypeStruct((rows, columns), gathered.dtype),
            jax.ShapeDtypeStruct((rows, probe.shape[1]), jnp.float32),
        ],
        compiler_params=pltpu.CompilerParams(vmem_limit_bytes=20 << 20),
    )(gathered, probe)


def shards(embed_rows, head_rows, row_offsets, slot_table, probe):
    probe = pltpu.with_memory_space_constraint(probe, pltpu.VMEM)
    embed_rows, head_rows, row_offsets, slot_table = (
        pltpu.with_memory_space_constraint(a, pltpu.HBM)
        for a in (embed_rows, head_rows, row_offsets, slot_table)
    )
    gathered = save(embed_rows, head_rows, row_offsets, slot_table)
    stored, sketch = finish(gathered, probe)
    return (stored.reshape(-1, BLOCK, stored.shape[1]), sketch.reshape(-1, BLOCK, sketch.shape[1]))


def solution(mesh):
    return jax.shard_map(
        shards,
        mesh=mesh,
        in_specs=(P("tensor", "dp"), P("tensor", "dp"), P(), P(), P()),
        out_specs=(P(("dp", "tensor"), None, None), P(("dp", "tensor"), None, None)),
        check_vma=False,
    )
```

```python
import functools
import itertools
import random

import jax
import jax.numpy as jnp
from jax import lax
from jax.experimental import pallas as pl
from jax.experimental.pallas import tpu as pltpu
from jax.sharding import PartitionSpec as P

R = 8192
BLOCK = 128
MESH = pl.DeviceIdType.MESH
Z = 4
Y = 4
X = 4
QUARTER = R // 4
LIFT = 16
TRAIL = QUARTER + LIFT
HIGH = R - QUARTER
PAD = BLOCK
OWN = PAD + R + QUARTER
FOREIGN = PAD + TRAIL
STEP = 3 * LIFT
UNROLL = 4
PIECES = ((0, 0, TRAIL), (1, 0, 32 * STEP), (1, 32 * STEP, 11 * STEP))
ROUNDS = (0, 4, 8) + tuple(range(16, 129, 8))


def exchange_order():
    offsets = list(itertools.product(range(Z), range(2), range(Y), range(X)))[1:]
    random.Random(1).shuffle(offsets)
    offsets.sort(key=lambda o: -sum(min(a, 4 - a) for a in (o[0], o[2], o[3])))
    return offsets + [(0, 0, 0, 0)]


ORDER = exchange_order()


def save_kernel(
    offsets_hbm, table_hbm, embed, head, gathered, offsets, table, incoming, lookup, picked, low, high_embed, high_head, own, arrived, foreign, trail, packed,
    load_sem, shift_send, shift_recv, scalar_sem, send_sem, recv_sem, plane_sem, space_sem,
):
    data = lax.axis_index("dp")
    tensor = lax.axis_index("tensor")
    me = data * (Y * X) + tensor
    z, core, y, x = data // 2, data % 2, tensor // X, tensor % X
    ranks = Y * X
    following = (data, (tensor + 1) % ranks)
    previous = (data, (tensor + ranks - 1) % ranks)

    def peer(offset):
        dz, dc, dy, dx = offset
        return (((z + dz) % Z) * 2 + (core + dc) % 2, ((y + dy) % Y) * X + (x + dx) % X)

    def signal(sem, device):
        pl.semaphore_signal(sem, inc=1, device_id=device, device_id_type=MESH)

    sources = (embed, head)
    high = (high_embed, high_head)
    height = embed.shape[0]

    def load(m, part):
        if part == 0:
            return pltpu.make_async_copy(
                sources[m].at[pl.ds(HIGH, height - HIGH)],
                high[m],
                load_sem.at[0, m],
            )
        return pltpu.make_async_copy(sources[m].at[pl.ds(0, HIGH)], low.at[m], load_sem.at[1, m])

    row = [(0, dc, 0, dx) for dc in range(2) for dx in range(X) if (dc, dx) != (0, 0)]
    column = [(0, 0, d, 0) for d in range(1, Y)]
    stack = [(d, 0, 0, 0) for d in range(1, Z)]
    barrier = pltpu.get_barrier_semaphore()
    signal(barrier, following)
    signal(barrier, previous)
    for offset in stack + column + row:
        signal(barrier, peer(offset))
    scalars = [
        pltpu.make_async_copy(offsets_hbm, offsets, scalar_sem.at[0]),
        pltpu.make_async_copy(table_hbm, table, scalar_sem.at[1]),
    ]
    for copy in scalars:
        copy.start()
    load(0, 0).start()
    load(1, 0).start()
    pl.semaphore_wait(barrier, 2 + len(stack + column + row))

    def shift(side, piece):
        m, first, rows = PIECES[piece]
        if side == 0:
            source = trail.at[m, pl.ds(first, rows)]
        else:
            rows = min(rows, QUARTER - first)
            source = sources[m].at[pl.ds(first, rows)]
        return pltpu.make_async_remote_copy(
            src_ref=source,
            dst_ref=arrived.at[m, side, pl.ds(first, rows)],
            send_sem=shift_send.at[side, piece],
            recv_sem=shift_recv.at[side, piece],
            device_id=(following, previous)[side],
            device_id_type=MESH,
        )

    for piece in range(len(PIECES)):
        shift(1, piece).start()
    scalars[0].wait()
    for m in range(2):
        load(m, 0).wait()
        begin = (tensor + 1) * R - offsets[m, tensor] - HIGH
        begin = jnp.clip(begin, 0, height - HIGH - TRAIL + LIFT - 1)
        begin = lax.div(begin, LIFT) * LIFT
        trail[m] = high[m][pl.ds(begin, TRAIL), :]
        load(m, 1).start()
        for piece in range(len(PIECES)):
            if PIECES[piece][0] == m:
                shift(0, piece).start()
    scalars[1].wait()

    for offset in column:
        signal(plane_sem, peer(offset))
    pl.semaphore_wait(plane_sem, len(column))
    for offset in stack:
        signal(space_sem, peer(offset))
    per_rank = R // BLOCK
    slots = table.shape[0] // len(ORDER)

    @pl.loop(0, len(ORDER))
    def _(j):
        total = jnp.int32(0)
        for s in range(slots):
            number = table[j * slots + s]
            half = lax.div(number, per_rank * ranks)
            block = lax.rem(number, per_rank)
            rank = lax.rem(lax.div(number, per_rank), ranks)
            other = jnp.minimum(jnp.abs(rank - tensor), 1)
            total += (half * per_rank + block) * (1 - other)
        picked[j] = jnp.clip(total, 0, 2 * per_rank - 1)

    for k, offset in enumerate(ORDER):
        to = peer(offset)
        lookup[k] = to[0] * ranks + to[1]

    load(0, 1).wait()
    load(1, 1).wait()
    step = 256
    for m in range(2):

        @pl.loop(0, HIGH // step)
        def _(i):
            at = pl.multiple_of(i * step, step)
            own[pl.ds(m * OWN + PAD + at, step), :] = low[m, pl.ds(at, step), :].astype(jnp.float32)

        @pl.loop(0, (R + QUARTER - HIGH) // step)
        def _(i):
            at = pl.multiple_of(i * step, step)
            rows = high[m][pl.ds(at, step), :]
            own[pl.ds(m * OWN + PAD + HIGH + at, step), :] = rows.astype(jnp.float32)

    pl.semaphore_wait(space_sem, len(stack))

    for piece, (m, first_row, rows) in enumerate(PIECES):
        for side in range(2):
            shift(side, piece).wait_recv()

            @pl.loop(0, rows // STEP)
            def _(i):
                at = pl.multiple_of(first_row + i * STEP, LIFT)
                rows = arrived[m, side, pl.ds(at, STEP), :].astype(jnp.float32)
                foreign[pl.ds((m * 2 + side) * FOREIGN + PAD + at, STEP), :] = rows

    earlier = (tensor + ranks - 1) % ranks
    befores = [offsets[m, tensor] - tensor * R for m in range(2)]
    afters = [offsets[m, tensor + 1] - tensor * R for m in range(2)]
    lifts = [lax.rem((earlier + 1) * R - offsets[m, earlier], LIFT) for m in range(2)]
    local_row = lax.broadcasted_iota(jnp.int32, (BLOCK, embed.shape[1]), 0)

    def pack(k):
        local = picked[lookup[k]]
        m = lax.div(local, per_rank)
        block = lax.rem(local, per_rank)
        first = block * BLOCK
        before = befores[0] + m * (befores[1] - befores[0])
        after = afters[0] + m * (afters[1] - afters[0])
        lift = lifts[0] + m * (lifts[1] - lifts[0])
        own_at = m * OWN + PAD + jnp.clip(first - before, -PAD, R + QUARTER - BLOCK)
        left_at = jnp.clip(first + lift, -PAD, TRAIL - BLOCK)
        right_at = jnp.clip(first - after, -PAD, TRAIL - BLOCK)
        side = lax.div(block, per_rank // 2)
        at = (m * 2 + side) * FOREIGN + PAD + left_at + side * (right_at - left_at)
        mine = own[pl.ds(own_at, BLOCK), :]
        theirs = foreign[pl.ds(at, BLOCK), :]
        keep = (local_row >= before - first) & (local_row < after - first)
        packed[k] = jnp.where(keep, mine, theirs).astype(packed.dtype)

    def send(k):
        return pltpu.make_async_remote_copy(
            src_ref=packed.at[k],
            dst_ref=incoming.at[me],
            send_sem=send_sem,
            recv_sem=recv_sem,
            device_id=peer(ORDER[k]),
            device_id_type=MESH,
        )

    count = len(ORDER)
    for start, stop, behind in zip(ROUNDS, ROUNDS[1:] + (count,), (0,) + ROUNDS):
        if start < stop:

            @pl.loop(start, stop, unroll=UNROLL)
            def _(k):
                pack(k)

        for k in range(behind, min(start, count - 1)):
            send(k).start()
    incoming[me] = packed[count - 1]
    everything = packed.at[pl.ds(0, count - 1)]
    pltpu.make_async_copy(everything, everything, recv_sem).wait()
    width = embed.shape[1]

    @pl.loop(0, slots, unroll=2)
    def _(slot):
        rank = lax.rem(lax.div(table[me * slots + slot], per_rank), ranks)
        at = pl.ds(pl.multiple_of(slot * BLOCK, BLOCK), BLOCK)
        for d in range(2 * Z):
            gathered[at, d * width:(d + 1) * width] = incoming[d * ranks + rank]

    pltpu.make_async_copy(everything, everything, send_sem).wait()
    for piece in range(len(PIECES)):
        for side in range(2):
            shift(side, piece).wait_send()


def save(embed_rows, head_rows, row_offsets, slot_table):
    height, width = embed_rows.shape
    dtype = embed_rows.dtype
    slots = slot_table.shape[0] // len(ORDER)
    return pl.pallas_call(
        save_kernel,
        in_specs=[pl.BlockSpec(memory_space=pl.ANY)] * 4,
        out_specs=pl.BlockSpec(memory_space=pltpu.VMEM),
        scratch_shapes=[
            pltpu.SMEM(row_offsets.shape, jnp.int32),
            pltpu.SMEM(slot_table.shape, jnp.int32),
            pltpu.VMEM((len(ORDER), BLOCK, width), dtype),
            pltpu.SMEM((len(ORDER),), jnp.int32),
            pltpu.SMEM((len(ORDER),), jnp.int32),
            pltpu.VMEM((2, HIGH, width), dtype),
            pltpu.VMEM((height - HIGH, width), dtype),
            pltpu.VMEM((height - HIGH, width), dtype),
            pltpu.VMEM((2 * OWN, width), jnp.float32),
            pltpu.VMEM((2, 2, TRAIL, width), dtype),
            pltpu.VMEM((4 * FOREIGN, width), jnp.float32),
            pltpu.VMEM((2, TRAIL, width), dtype),
            pltpu.VMEM((len(ORDER), BLOCK, width), dtype),
            pltpu.SemaphoreType.DMA((2, 2)),
            pltpu.SemaphoreType.DMA((2, len(PIECES))),
            pltpu.SemaphoreType.DMA((2, len(PIECES))),
            pltpu.SemaphoreType.DMA((2,)),
            pltpu.SemaphoreType.DMA,
            pltpu.SemaphoreType.DMA,
            pltpu.SemaphoreType.REGULAR,
            pltpu.SemaphoreType.REGULAR,
        ],
        out_shape=pltpu.VMEM((slots * BLOCK, 2 * Z * width), dtype),
        compiler_params=pltpu.CompilerParams(
            collective_id=0, has_side_effects=True, vmem_limit_bytes=38 << 20
        ),
    )(row_offsets, slot_table, embed_rows, head_rows)


ROWS = 256
BUFFERS = 4


def finish_kernel(gathered, weights, stored, sketch, product, stored_sem, sketch_sem):
    groups = gathered.shape[0] // ROWS

    def put_stored(g):
        at = pl.ds(g * ROWS, ROWS)
        return pltpu.make_async_copy(gathered.at[at], stored.at[at], stored_sem.at[g])

    def put_sketch(g):
        return pltpu.make_async_copy(
            product.at[g % BUFFERS], sketch.at[pl.ds(g * ROWS, ROWS)], sketch_sem.at[g]
        )

    for g in range(groups):
        put_stored(g).start()
    for g in range(groups):
        if g >= BUFFERS:
            put_sketch(g - BUFFERS).wait()
        x = gathered[g * ROWS:(g + 1) * ROWS]
        product[g % BUFFERS] = jnp.dot(x, weights[...], preferred_element_type=jnp.float32)
        put_sketch(g).start()
    for g in range(groups):
        put_stored(g).wait()
    for g in range(groups - BUFFERS, groups):
        put_sketch(g).wait()


def finish(gathered, probe):
    rows, columns = gathered.shape
    return pl.pallas_call(
        finish_kernel,
        in_specs=[pl.BlockSpec(memory_space=pltpu.VMEM)] * 2,
        out_specs=[pl.BlockSpec(memory_space=pl.ANY)] * 2,
        scratch_shapes=[
            pltpu.VMEM((BUFFERS, ROWS, probe.shape[1]), jnp.float32),
            pltpu.SemaphoreType.DMA((rows // ROWS,)),
            pltpu.SemaphoreType.DMA((rows // ROWS,)),
        ],
        out_shape=[
            jax.ShapeDtypeStruct((rows, columns), gathered.dtype),
            jax.ShapeDtypeStruct((rows, probe.shape[1]), jnp.float32),
        ],
        compiler_params=pltpu.CompilerParams(vmem_limit_bytes=20 << 20),
    )(gathered, probe)


def shards(embed_rows, head_rows, row_offsets, slot_table, probe):
    probe = pltpu.with_memory_space_constraint(probe, pltpu.VMEM)
    embed_rows, head_rows, row_offsets, slot_table = (
        pltpu.with_memory_space_constraint(a, pltpu.HBM)
        for a in (embed_rows, head_rows, row_offsets, slot_table)
    )
    gathered = save(embed_rows, head_rows, row_offsets, slot_table)
    stored, sketch = finish(gathered, probe)
    return (stored.reshape(-1, BLOCK, stored.shape[1]), sketch.reshape(-1, BLOCK, sketch.shape[1]))


def solution(mesh):
    return jax.shard_map(
        shards,
        mesh=mesh,
        in_specs=(P("tensor", "dp"), P("tensor", "dp"), P(), P(), P()),
        out_specs=(P(("dp", "tensor"), None, None), P(("dp", "tensor"), None, None)),
        check_vma=False,
    )
```

```python
import functools
import itertools
import random

import jax
import jax.numpy as jnp
from jax import lax
from jax.experimental import pallas as pl
from jax.experimental.pallas import tpu as pltpu
from jax.sharding import PartitionSpec as P

R = 8192
BLOCK = 128
MESH = pl.DeviceIdType.MESH
Z = 4
Y = 4
X = 4
QUARTER = R // 4
LIFT = 16
TRAIL = QUARTER + LIFT
HIGH = R - QUARTER
PAD = BLOCK
OWN = PAD + R + QUARTER
FOREIGN = PAD + TRAIL
STEP = 3 * LIFT
UNROLL = 4
PIECES = ((0, 0, TRAIL), (1, 0, 32 * STEP), (1, 32 * STEP, 11 * STEP))
ROUNDS = (0, 4, 8) + tuple(range(16, 129, 8))


def exchange_order():
    offsets = list(itertools.product(range(Z), range(2), range(Y), range(X)))[1:]
    random.Random(1).shuffle(offsets)
    offsets.sort(key=lambda o: -sum(min(a, 4 - a) for a in (o[0], o[2], o[3])))
    return offsets + [(0, 0, 0, 0)]


ORDER = exchange_order()


def save_kernel(
    offsets_hbm, table_hbm, embed, head, gathered, offsets, table, incoming, lookup, picked, low, high_embed, high_head, own, arrived, foreign, trail, packed,
    load_sem, shift_send, shift_recv, scalar_sem, send_sem, recv_sem, plane_sem, space_sem,
):
    data = lax.axis_index("dp")
    tensor = lax.axis_index("tensor")
    me = data * (Y * X) + tensor
    z, core, y, x = data // 2, data % 2, tensor // X, tensor % X
    ranks = Y * X
    following = (data, (tensor + 1) % ranks)
    previous = (data, (tensor + ranks - 1) % ranks)

    def peer(offset):
        dz, dc, dy, dx = offset
        return (((z + dz) % Z) * 2 + (core + dc) % 2, ((y + dy) % Y) * X + (x + dx) % X)

    def target(offset):
        dz, dc, dy, dx = offset
        dz, dy, dx = (dz + core * (dy - dz), dy + core * (dx - dy), dx + core * (dz - dx))
        return (((z + dz) % Z) * 2 + (core + dc) % 2, ((y + dy) % Y) * X + (x + dx) % X)

    def signal(sem, device):
        pl.semaphore_signal(sem, inc=1, device_id=device, device_id_type=MESH)

    sources = (embed, head)
    high = (high_embed, high_head)
    height = embed.shape[0]

    def load(m, part):
        if part == 0:
            return pltpu.make_async_copy(
                sources[m].at[pl.ds(HIGH, height - HIGH)],
                high[m],
                load_sem.at[0, m],
            )
        return pltpu.make_async_copy(sources[m].at[pl.ds(0, HIGH)], low.at[m], load_sem.at[1, m])

    row = [(0, dc, 0, dx) for dc in range(2) for dx in range(X) if (dc, dx) != (0, 0)]
    column = [(0, 0, d, 0) for d in range(1, Y)]
    stack = [(d, 0, 0, 0) for d in range(1, Z)]
    barrier = pltpu.get_barrier_semaphore()
    signal(barrier, following)
    signal(barrier, previous)
    for offset in stack + column + row:
        signal(barrier, peer(offset))
    scalars = [
        pltpu.make_async_copy(offsets_hbm, offsets, scalar_sem.at[0]),
        pltpu.make_async_copy(table_hbm, table, scalar_sem.at[1]),
    ]
    for copy in scalars:
        copy.start()
    load(0, 0).start()
    load(1, 0).start()
    pl.semaphore_wait(barrier, 2 + len(stack + column + row))

    def shift(side, piece):
        m, first, rows = PIECES[piece]
        if side == 0:
            source = trail.at[m, pl.ds(first, rows)]
        else:
            rows = min(rows, QUARTER - first)
            source = sources[m].at[pl.ds(first, rows)]
        return pltpu.make_async_remote_copy(
            src_ref=source,
            dst_ref=arrived.at[m, side, pl.ds(first, rows)],
            send_sem=shift_send.at[side, piece],
            recv_sem=shift_recv.at[side, piece],
            device_id=(following, previous)[side],
            device_id_type=MESH,
        )

    for piece in range(len(PIECES)):
        shift(1, piece).start()
    scalars[0].wait()
    for m in range(2):
        load(m, 0).wait()
        begin = (tensor + 1) * R - offsets[m, tensor] - HIGH
        begin = jnp.clip(begin, 0, height - HIGH - TRAIL + LIFT - 1)
        begin = lax.div(begin, LIFT) * LIFT
        trail[m] = high[m][pl.ds(begin, TRAIL), :]
        load(m, 1).start()
        for piece in range(len(PIECES)):
            if PIECES[piece][0] == m:
                shift(0, piece).start()
    scalars[1].wait()

    for offset in column:
        signal(plane_sem, peer(offset))
    pl.semaphore_wait(plane_sem, len(column))
    for offset in stack:
        signal(space_sem, peer(offset))
    per_rank = R // BLOCK
    slots = table.shape[0] // len(ORDER)

    @pl.loop(0, len(ORDER))
    def _(j):
        total = jnp.int32(0)
        for s in range(slots):
            number = table[j * slots + s]
            half = lax.div(number, per_rank * ranks)
            block = lax.rem(number, per_rank)
            rank = lax.rem(lax.div(number, per_rank), ranks)
            other = jnp.minimum(jnp.abs(rank - tensor), 1)
            total += (half * per_rank + block) * (1 - other)
        picked[j] = jnp.clip(total, 0, 2 * per_rank - 1)

    for k, offset in enumerate(ORDER):
        to = target(offset)
        lookup[k] = to[0] * ranks + to[1]

    load(0, 1).wait()
    load(1, 1).wait()
    step = 256
    for m in range(2):

        @pl.loop(0, HIGH // step)
        def _(i):
            at = pl.multiple_of(i * step, step)
            own[pl.ds(m * OWN + PAD + at, step), :] = low[m, pl.ds(at, step), :].astype(jnp.float32)

        @pl.loop(0, (R + QUARTER - HIGH) // step)
        def _(i):
            at = pl.multiple_of(i * step, step)
            rows = high[m][pl.ds(at, step), :]
            own[pl.ds(m * OWN + PAD + HIGH + at, step), :] = rows.astype(jnp.float32)

    pl.semaphore_wait(space_sem, len(stack))

    for piece, (m, first_row, rows) in enumerate(PIECES):
        for side in range(2):
            shift(side, piece).wait_recv()

            @pl.loop(0, rows // STEP)
            def _(i):
                at = pl.multiple_of(first_row + i * STEP, LIFT)
                rows = arrived[m, side, pl.ds(at, STEP), :].astype(jnp.float32)
                foreign[pl.ds((m * 2 + side) * FOREIGN + PAD + at, STEP), :] = rows

    earlier = (tensor + ranks - 1) % ranks
    befores = [offsets[m, tensor] - tensor * R for m in range(2)]
    afters = [offsets[m, tensor + 1] - tensor * R for m in range(2)]
    lifts = [lax.rem((earlier + 1) * R - offsets[m, earlier], LIFT) for m in range(2)]
    local_row = lax.broadcasted_iota(jnp.int32, (BLOCK, embed.shape[1]), 0)

    def pack(k):
        local = picked[lookup[k]]
        m = lax.div(local, per_rank)
        block = lax.rem(local, per_rank)
        first = block * BLOCK
        before = befores[0] + m * (befores[1] - befores[0])
        after = afters[0] + m * (afters[1] - afters[0])
        lift = lifts[0] + m * (lifts[1] - lifts[0])
        own_at = m * OWN + PAD + jnp.clip(first - before, -PAD, R + QUARTER - BLOCK)
        left_at = jnp.clip(first + lift, -PAD, TRAIL - BLOCK)
        right_at = jnp.clip(first - after, -PAD, TRAIL - BLOCK)
        side = lax.div(block, per_rank // 2)
        at = (m * 2 + side) * FOREIGN + PAD + left_at + side * (right_at - left_at)
        mine = own[pl.ds(own_at, BLOCK), :]
        theirs = foreign[pl.ds(at, BLOCK), :]
        keep = (local_row >= before - first) & (local_row < after - first)
        packed[k] = jnp.where(keep, mine, theirs).astype(packed.dtype)

    def send(k):
        return pltpu.make_async_remote_copy(
            src_ref=packed.at[k],
            dst_ref=incoming.at[me],
            send_sem=send_sem,
            recv_sem=recv_sem,
            device_id=target(ORDER[k]),
            device_id_type=MESH,
        )

    count = len(ORDER)
    for start, stop, behind in zip(ROUNDS, ROUNDS[1:] + (count,), (0,) + ROUNDS):
        if start < stop:

            @pl.loop(start, stop, unroll=UNROLL)
            def _(k):
                pack(k)

        for k in range(behind, min(start, count - 1)):
            send(k).start()
    incoming[me] = packed[count - 1]
    everything = packed.at[pl.ds(0, count - 1)]
    pltpu.make_async_copy(everything, everything, recv_sem).wait()
    width = embed.shape[1]

    @pl.loop(0, slots, unroll=2)
    def _(slot):
        rank = lax.rem(lax.div(table[me * slots + slot], per_rank), ranks)
        at = pl.ds(pl.multiple_of(slot * BLOCK, BLOCK), BLOCK)
        for d in range(2 * Z):
            gathered[at, d * width:(d + 1) * width] = incoming[d * ranks + rank]

    pltpu.make_async_copy(everything, everything, send_sem).wait()
    for piece in range(len(PIECES)):
        for side in range(2):
            shift(side, piece).wait_send()


def save(embed_rows, head_rows, row_offsets, slot_table):
    height, width = embed_rows.shape
    dtype = embed_rows.dtype
    slots = slot_table.shape[0] // len(ORDER)
    return pl.pallas_call(
        save_kernel,
        in_specs=[pl.BlockSpec(memory_space=pl.ANY)] * 4,
        out_specs=pl.BlockSpec(memory_space=pltpu.VMEM),
        scratch_shapes=[
            pltpu.SMEM(row_offsets.shape, jnp.int32),
            pltpu.SMEM(slot_table.shape, jnp.int32),
            pltpu.VMEM((len(ORDER), BLOCK, width), dtype),
            pltpu.SMEM((len(ORDER),), jnp.int32),
            pltpu.SMEM((len(ORDER),), jnp.int32),
            pltpu.VMEM((2, HIGH, width), dtype),
            pltpu.VMEM((height - HIGH, width), dtype),
            pltpu.VMEM((height - HIGH, width), dtype),
            pltpu.VMEM((2 * OWN, width), jnp.float32),
            pltpu.VMEM((2, 2, TRAIL, width), dtype),
            pltpu.VMEM((4 * FOREIGN, width), jnp.float32),
            pltpu.VMEM((2, TRAIL, width), dtype),
            pltpu.VMEM((len(ORDER), BLOCK, width), dtype),
            pltpu.SemaphoreType.DMA((2, 2)),
            pltpu.SemaphoreType.DMA((2, len(PIECES))),
            pltpu.SemaphoreType.DMA((2, len(PIECES))),
            pltpu.SemaphoreType.DMA((2,)),
            pltpu.SemaphoreType.DMA,
            pltpu.SemaphoreType.DMA,
            pltpu.SemaphoreType.REGULAR,
            pltpu.SemaphoreType.REGULAR,
        ],
        out_shape=pltpu.VMEM((slots * BLOCK, 2 * Z * width), dtype),
        compiler_params=pltpu.CompilerParams(
            collective_id=0, has_side_effects=True, vmem_limit_bytes=38 << 20
        ),
    )(row_offsets, slot_table, embed_rows, head_rows)


ROWS = 256
BUFFERS = 4


def finish_kernel(gathered, weights, stored, sketch, product, stored_sem, sketch_sem):
    groups = gathered.shape[0] // ROWS

    def put_stored(g):
        at = pl.ds(g * ROWS, ROWS)
        return pltpu.make_async_copy(gathered.at[at], stored.at[at], stored_sem.at[g])

    def put_sketch(g):
        return pltpu.make_async_copy(
            product.at[g % BUFFERS], sketch.at[pl.ds(g * ROWS, ROWS)], sketch_sem.at[g]
        )

    for g in range(groups):
        put_stored(g).start()
    for g in range(groups):
        if g >= BUFFERS:
            put_sketch(g - BUFFERS).wait()
        x = gathered[g * ROWS:(g + 1) * ROWS]
        product[g % BUFFERS] = jnp.dot(x, weights[...], preferred_element_type=jnp.float32)
        put_sketch(g).start()
    for g in range(groups):
        put_stored(g).wait()
    for g in range(groups - BUFFERS, groups):
        put_sketch(g).wait()


def finish(gathered, probe):
    rows, columns = gathered.shape
    return pl.pallas_call(
        finish_kernel,
        in_specs=[pl.BlockSpec(memory_space=pltpu.VMEM)] * 2,
        out_specs=[pl.BlockSpec(memory_space=pl.ANY)] * 2,
        scratch_shapes=[
            pltpu.VMEM((BUFFERS, ROWS, probe.shape[1]), jnp.float32),
            pltpu.SemaphoreType.DMA((rows // ROWS,)),
            pltpu.SemaphoreType.DMA((rows // ROWS,)),
        ],
        out_shape=[
            jax.ShapeDtypeStruct((rows, columns), gathered.dtype),
            jax.ShapeDtypeStruct((rows, probe.shape[1]), jnp.float32),
        ],
        compiler_params=pltpu.CompilerParams(vmem_limit_bytes=20 << 20),
    )(gathered, probe)


def shards(embed_rows, head_rows, row_offsets, slot_table, probe):
    probe = pltpu.with_memory_space_constraint(probe, pltpu.VMEM)
    embed_rows, head_rows, row_offsets, slot_table = (
        pltpu.with_memory_space_constraint(a, pltpu.HBM)
        for a in (embed_rows, head_rows, row_offsets, slot_table)
    )
    gathered = save(embed_rows, head_rows, row_offsets, slot_table)
    stored, sketch = finish(gathered, probe)
    return (stored.reshape(-1, BLOCK, stored.shape[1]), sketch.reshape(-1, BLOCK, sketch.shape[1]))


def solution(mesh):
    return jax.shard_map(
        shards,
        mesh=mesh,
        in_specs=(P("tensor", "dp"), P("tensor", "dp"), P(), P(), P()),
        out_specs=(P(("dp", "tensor"), None, None), P(("dp", "tensor"), None, None)),
        check_vma=False,
    )
```
